128 devices in a mesh: graph: 32 (over z, x, core), batch: 4 (over y).
Axes of the slice: x: 4, y: 4, z: 4, core: 2. Of those that a mesh axis runs over, the one named last changes fastest.
Arguments:
- node_latent: bfloat16 [4, 4096, 512], P('batch', 'graph'), may hold values from -6 to 6
- edge_latent: bfloat16 [4, 32768, 512], P('batch', 'graph'), may hold values from -6 to 6
- node_cotangent: bfloat16 [4, 4096, 512], P('batch', 'graph'), may hold values from -6 to 6
- edge_w_in: bfloat16 [2, 1536, 512], replicated, may hold values from -0.15625 to 0.15625
- edge_w_out: bfloat16 [2, 512, 512], replicated, may hold values from -0.25 to 0.25
- node_w_in: bfloat16 [2, 1024, 512], replicated, may hold values from -0.1875 to 0.1875
- node_w_out: bfloat16 [2, 512, 512], replicated, may hold values from -0.25 to 0.25
- edge_gain: float32 [2, 512], replicated, may hold values from 0.25 to 1.75
- node_gain: float32 [2, 512], replicated, may hold values from 0.25 to 1.75
- edge_slot: int32 [32768], P('graph'), may hold values from 0 to 1151, as said below
- edge_receiver: int32 [32768], P('graph'), may hold values from 0 to 127
- send_list: int32 [1024, 32], P('graph'), may hold values from 0 to 127, as said below
- edge_count: int32 [32], P('graph'), may hold values from 256 to 1024, as said below
Outputs:
- node_out: float32 [4, 4096, 512], P('batch', 'graph')
- node_grad: float32 [4, 4096, 512], P('batch', 'graph')
- grad_edge_in: float32 [2, 1536, 512], P(None, ('graph', 'batch'))
- grad_edge_out: float32 [2, 512, 512], P(None, ('graph', 'batch'))
- grad_node_in: float32 [2, 1024, 512], P(None, ('graph', 'batch'))
- grad_node_out: float32 [2, 512, 512], P(None, ('graph', 'batch'))
- grad_edge_gain: float32 [2, 512], P(None, ('graph', 'batch'))
- grad_node_gain: float32 [2, 512], P(None, ('graph', 'batch'))
The draws below stay inside these ranges and needn't reach their ends.
Inputs may be any that keep to these rules, and one draw needn't show every extreme that they name: `edge_slot`: for edge j of partition p = j // 1024: a slot below 128 names a node of partition p; a slot s of 128 or more names row (s - 128) % 32 of the list that partition q = (s - 128) // 32 keeps for partition p, and q differs from p cyclically by 1 to 2 steps or by exactly 32 // 2 steps. `edge_receiver`: the receiving node is a node of the edge's own partition. `send_list`: row q * 32 + p holds 32 distinct node numbers within partition q, the nodes whose latents partition p may read. `edge_count`: edge slots at or above a partition's count carry no edge.
All inputs are finite; a program needn't handle non-finite values.
Results may differ from the reference program's by a relative error of at most 0.035.
Values may be sent and summed in bfloat16 or wider, within the bound.
A program may use at most 128 MiB of HBM per device.

```python
import jax
import jax.numpy as jnp
from jax import lax

D = 512
HID = 512
LAYERS = 2
HOPS = 2
NOD_DEV = 128
EDGE_CAP = 1024
PEER_CAP = 32
NODES = 4096
EDGES = 32768
SAMPLES = 4
N_GRAPH = 32


def draw_edge_slot(key, part):
    subkeys = jax.random.split(jax.random.fold_in(key, 11), 4)
    edge_ids = jnp.arange(EDGES, dtype=jnp.int32)
    owner = edge_ids // EDGE_CAP
    is_local = jax.random.randint(subkeys[0], (EDGES,), 0, 2) == 0
    local_slot = jax.random.randint(subkeys[1], (EDGES,), 0, NOD_DEV)
    hop_pick = jax.random.randint(subkeys[2], (EDGES,), 0, 2 * HOPS + 1)
    offset = jnp.where(hop_pick < HOPS, hop_pick - HOPS, jnp.where(hop_pick < 2 * HOPS, hop_pick - HOPS + 1, N_GRAPH // 2))
    source = (owner + offset) % N_GRAPH
    within = jax.random.randint(subkeys[3], (EDGES,), 0, PEER_CAP)
    return jnp.where(is_local, local_slot, NOD_DEV + source * PEER_CAP + within).astype(jnp.int32)


def draw_send_list(key, part):
    subkeys = jax.random.split(jax.random.fold_in(key, 23), N_GRAPH * N_GRAPH)

    def one_list(row_key):
        return jax.random.permutation(row_key, NOD_DEV)[:PEER_CAP]
    return jax.vmap(one_list)(subkeys).astype(jnp.int32)


def draw_edge_count(key, part):
    subkeys = jax.random.split(jax.random.fold_in(key, 37), 2)
    counts = jax.random.randint(subkeys[0], (N_GRAPH,), EDGE_CAP // 4, EDGE_CAP + 1)
    fullest = jax.random.randint(subkeys[1], (), 0, N_GRAPH)
    return jnp.where(jnp.arange(N_GRAPH) == fullest, EDGE_CAP, counts).astype(jnp.int32)


def with_ends(array, stream_key, smallest, top_value):
    shape = array.shape
    index_at = [jax.random.randint(jax.random.fold_in(stream_key, axis), (), 0, shape[axis]) for axis in range(len(shape))]
    array = array.at[tuple(index_at)].set(smallest)
    longest = shape.index(max(shape))
    index_at[longest] = (index_at[longest] + 1) % shape[longest]
    return array.at[tuple(index_at)].set(top_value)


def shard_levels(stream_key, shape, cuts, low, largest):
    level = 1.0
    for position, blocks in cuts:
        heights = jax.random.uniform(jax.random.fold_in(jax.random.fold_in(stream_key, 6), position), (blocks,), jnp.float32, low / len(cuts), largest / len(cuts))
        level = level * jnp.repeat(jnp.exp(heights), shape[position] // blocks).reshape((-1,) + (1,) * (len(shape) - 1 - position))
    return level


def noise(own_key, shape, spread, most, cuts=(), held_as=jnp.bfloat16):
    array = spread * jax.random.normal(own_key, shape, jnp.float32)
    if cuts:
        array = array * shard_levels(own_key, shape, cuts, -0.22, 0.18)
    return jnp.clip(array, -most, most).astype(held_as)


def setup_inputs(seed: int = 0) -> dict:
    keys = jax.random.split(jax.random.key(seed), 14)
    node_latent = noise(keys[0], (SAMPLES, NODES, D), 1.0, 6.0, ((0, 4), (1, 32)))
    edge_latent = noise(keys[1], (SAMPLES, EDGES, D), 1.0, 6.0, ((0, 4), (1, 32)))
    node_cotangent = noise(keys[2], (SAMPLES, NODES, D), 1.0, 6.0, ((0, 4), (1, 32)))
    edge_w_in = noise(keys[3], (LAYERS, 3 * D, HID), (3 * D) ** -0.5, 0.15625)
    edge_w_out = noise(keys[4], (LAYERS, HID, D), HID ** -0.5, 0.25)
    node_w_in = noise(keys[5], (LAYERS, 2 * D, HID), (2 * D) ** -0.5, 0.1875)
    node_w_out = noise(keys[6], (LAYERS, HID, D), HID ** -0.5, 0.25)
    edge_gain = jnp.clip(1.0 + 0.15 * jax.random.normal(keys[7], (LAYERS, D), jnp.float32), 0.25, 1.75)
    node_gain = jnp.clip(1.0 + 0.15 * jax.random.normal(keys[8], (LAYERS, D), jnp.float32), 0.25, 1.75)
    edge_slot = draw_edge_slot(jax.random.fold_in(keys[13], 71), 0)
    edge_receiver = with_ends(jax.random.randint(keys[10], (EDGES,), 0, NOD_DEV), jax.random.fold_in(keys[10], 1), 0, NOD_DEV - 1).astype(jnp.int32)
    send_list = draw_send_list(jax.random.fold_in(keys[13], 71), 0)
    edge_count = draw_edge_count(jax.random.fold_in(keys[13], 71), 0)
    return {"node_latent": node_latent, "edge_latent": edge_latent, "node_cotangent": node_cotangent, "edge_w_in": edge_w_in, "edge_w_out": edge_w_out, "node_w_in": node_w_in, "node_w_out": node_w_out, "edge_gain": edge_gain, "node_gain": node_gain, "edge_slot": edge_slot, "edge_receiver": edge_receiver, "send_list": send_list, "edge_count": edge_count}


EPSILON = 1e-05

def mlp_forward(pieces, weights, w_out, gain, live):
    pre_act = None
    for piece, weight in zip(pieces, weights):
        term = jnp.dot(piece, weight, preferred_element_type=jnp.float32)
        pre_act = term if pre_act is None else pre_act + term
    hidden = (pre_act * jax.nn.sigmoid(pre_act)).astype(jnp.bfloat16)
    projected = jnp.dot(hidden, w_out, preferred_element_type=jnp.float32)
    centre = projected - lax.optimization_barrier(jnp.mean(projected, axis=-1, keepdims=True))
    inv_std = lax.rsqrt(lax.optimization_barrier(jnp.mean(centre * centre, axis=-1, keepdims=True)) + EPSILON)
    normed = centre * inv_std
    result = normed * gain
    if live is not None:
        result = result * live[:, None]
    return (result, (pre_act, hidden, normed, inv_std))

def mlp_backward(grad_out, pieces, weights, w_out, gain, live, saved):
    pre_act, hidden, normed, inv_std = saved
    if live is not None:
        grad_out = grad_out * live[:, None]
    grad_gain = lax.optimization_barrier(jnp.sum(grad_out * normed, axis=0))
    grad_norm = grad_out * gain
    grad_proj = inv_std * (grad_norm - lax.optimization_barrier(jnp.mean(grad_norm, axis=-1, keepdims=True)) - normed * lax.optimization_barrier(jnp.mean(grad_norm * normed, axis=-1, keepdims=True)))
    grad_proj_bf = grad_proj.astype(jnp.bfloat16)
    grad_w_out = jnp.dot(hidden.T, grad_proj_bf, preferred_element_type=jnp.float32)
    grad_hidden = jnp.dot(grad_proj_bf, w_out.T, preferred_element_type=jnp.float32)
    sigma = jax.nn.sigmoid(pre_act)
    grad_pre = grad_hidden * sigma * (1.0 + pre_act * (1.0 - sigma))
    grad_pre_bf = grad_pre.astype(jnp.bfloat16)
    grad_weights = [jnp.dot(piece.T, grad_pre_bf, preferred_element_type=jnp.float32) for piece in pieces]
    grad_pieces = [jnp.dot(grad_pre_bf, weight.T, preferred_element_type=jnp.float32) for weight in weights]
    return (grad_pieces, grad_weights, grad_w_out, grad_gain)

def run_sample(node_start, edge_start, cotangent, edge_w_in, edge_w_out, node_w_in, node_w_out, edge_gain, node_gain, sender, receiver, live):
    state = node_start.astype(jnp.float32)
    edge_state = edge_start.astype(jnp.float32)
    edge_bf = edge_start
    records = []
    for layer in range(LAYERS):
        node_bf = state.astype(jnp.bfloat16)
        if layer > 0:
            edge_bf = edge_state.astype(jnp.bfloat16)
        from_sender = node_bf[sender]
        at_receiver = node_bf[receiver]
        w_first = edge_w_in[layer]
        edge_weights = [w_first[:D], w_first[2 * D:], w_first[D:2 * D]]
        edge_inputs = [edge_bf, at_receiver, from_sender]
        message, edge_saved = mlp_forward(edge_inputs, edge_weights, edge_w_out[layer], edge_gain[layer], live)
        summed = jax.ops.segment_sum(message, receiver, num_segments=NODES).astype(jnp.bfloat16)
        n_first = node_w_in[layer]
        node_weights = [n_first[:D], n_first[D:]]
        node_inputs = [node_bf, summed]
        update, node_saved = mlp_forward(node_inputs, node_weights, node_w_out[layer], node_gain[layer], None)
        records.append((edge_inputs, edge_weights, edge_saved, node_inputs, node_weights, node_saved))
        edge_state = edge_state + message
        state = state + update
    grad_state = cotangent.astype(jnp.float32)
    grad_edge = None
    layer_grads = []
    for layer in reversed(range(LAYERS)):
        edge_inputs, edge_weights, edge_saved, node_inputs, node_weights, node_saved = records[layer]
        node_parts, node_wgrads, grad_n_out, grad_n_gain = mlp_backward(grad_state, node_inputs, node_weights, node_w_out[layer], node_gain[layer], None, node_saved)
        grad_message = node_parts[1][receiver]
        if grad_edge is not None:
            grad_message = grad_message + grad_edge
        edge_parts, edge_wgrads, grad_e_out, grad_e_gain = mlp_backward(grad_message, edge_inputs, edge_weights, edge_w_out[layer], edge_gain[layer], live, edge_saved)
        grad_edge = edge_parts[0] if grad_edge is None else edge_parts[0] + grad_edge
        grad_state = grad_state + node_parts[0] + jax.ops.segment_sum(edge_parts[1], receiver, num_segments=NODES) + jax.ops.segment_sum(edge_parts[2], sender, num_segments=NODES)
        grad_e_in = jnp.concatenate([edge_wgrads[0], edge_wgrads[2], edge_wgrads[1]], axis=0)
        grad_n_in = jnp.concatenate([node_wgrads[0], node_wgrads[1]], axis=0)
        layer_grads.append((grad_e_in, grad_e_out, grad_n_in, grad_n_out, grad_e_gain, grad_n_gain))
    layer_grads = layer_grads[::-1]
    stacked = tuple((jnp.stack([entry[index] for entry in layer_grads]) for index in range(6)))
    return (state, grad_state) + stacked

def reference(node_latent, edge_latent, node_cotangent, edge_w_in, edge_w_out, node_w_in, node_w_out, edge_gain, node_gain, edge_slot, edge_receiver, send_list, edge_count):
    edge_ids = jnp.arange(EDGES, dtype=jnp.int32)
    owner = edge_ids // EDGE_CAP
    is_local = edge_slot < NOD_DEV
    remote = jnp.where(is_local, 0, edge_slot - NOD_DEV).astype(jnp.int32)
    source = remote // PEER_CAP
    within = remote % PEER_CAP
    listed = send_list[source * N_GRAPH + owner, within]
    sender = jnp.where(is_local, owner * NOD_DEV + edge_slot, source * NOD_DEV + listed).astype(jnp.int32)
    receiver = (owner * NOD_DEV + edge_receiver).astype(jnp.int32)
    live = (edge_ids % EDGE_CAP < edge_count[owner]).astype(jnp.float32)

    def sample_fn(inputs):
        node_start, edge_start, cotangent = inputs
        return run_sample(node_start, edge_start, cotangent, edge_w_in, edge_w_out, node_w_in, node_w_out, edge_gain, node_gain, sender, receiver, live)
    results = lax.map(sample_fn, (node_latent, edge_latent, node_cotangent))
    node_out, node_grad = (results[0], results[1])
    sums = tuple((lax.optimization_barrier(jnp.sum(entry, axis=0)) for entry in results[2:]))
    return (node_out, node_grad, sums[0], sums[1], sums[2], sums[3], sums[4], sums[5])
```

```python
import types

import jax
import jax.numpy as jnp
from jax import lax
from jax.experimental import pallas as pl
from jax.experimental.pallas import tpu as pltpu
from jax.sharding import PartitionSpec as P

HOPS = 2
EPSILON = 1e-05
BF = jnp.bfloat16
F32 = jnp.float32
D = 512
NODES = 128
EDGES = 1024
PEER = 32
GROUP = 32
SAMPLES = 4
VMEM_LIMIT = 62 * 1024 * 1024
OFFSETS = tuple(o for o in range(-HOPS, HOPS + 1) if o != 0) + (GROUP // 2,)
HALO = len(OFFSETS) * PEER
RECV_AT = NODES
HALO_AT = 2 * NODES
SUMS_AT = 2 * NODES
FIRST, FORE, BACK = 1024, 1024, 512
FORE_UNROLL, BACK_UNROLL = 1, 1
MESH = pl.DeviceIdType.MESH
STREAM_TILES = (((16, 512),) * 3, ((8, 384), (8, 384), (24, 128)))
PART_ORDER = ((1, 2, 0), (2, 0, 1), (0, 1, 2))
AXES = ("graph", "batch")
scope = jax.named_scope


def dot(a, b):
    return jnp.dot(a, b, preferred_element_type=F32)


def dot_tb(a, b):
    return lax.dot_general(a, b, (((1,), (1,)), ((), ())), preferred_element_type=F32)


def dot_ta(a, b):
    return lax.dot_general(a, b, (((0,), (0,)), ((), ())), preferred_element_type=F32)


def place_id(graph, batch):
    return dict(zip(AXES, (graph, batch)))


def wrap(value, size):
    return lax.rem(value + 2 * size, size)


def iota(shape, dim):
    return lax.broadcasted_iota(jnp.int32, shape, dim)


def half_shape(part):
    first, second, _ = PART_ORDER[part]
    shape = [4, 4, 4]
    shape[second] = 2
    del shape[first]
    return tuple(shape)


NL, EWI, EL, EWO, NWI, NWO, COT = 0, (1, 6), 2, (3, 7), (4, 8), (5, 9), 10


def scratch_spec():
    vm = pltpu.VMEM

    def two(shape, dtype):
        return [vm(shape, dtype), vm(shape, dtype)]

    def parts(shape):
        keys = [(stream, part) for stream in range(2) for part in range(3)]
        return {key: vm(shape(key[1]) + STREAM_TILES[key[0]][key[1]], BF) for key in keys}

    return dict(
        nl=vm((NODES, D), BF),
        el=vm((EDGES, D), BF),
        ewi=vm((2, 3 * D, D), BF),
        ewo=vm((2, D, D), BF),
        nwi=vm((2, 2 * D, D), BF),
        nwo=vm((2, D, D), BF),
        cot=vm((NODES, D), BF),
        cnt=pltpu.SMEM((1,), jnp.int32),
        SR=vm((EDGES, 512), BF),
        SRT=vm((512, EDGES), BF),
        LT=vm((NODES, HALO), BF),
        PS=vm((512, D), BF),
        PRE=vm((EDGES, D), F32),
        EB1=vm((EDGES, D), BF),
        VB1=vm((NODES, D), BF),
        V1=vm((NODES, D), F32),
        N=two((EDGES, D), BF),
        DA=two((EDGES, D), BF),
        H=two((EDGES, D), BF),
        INV=two((EDGES, 1), F32),
        NN=two((NODES, D), F32),
        NDA=two((NODES, D), F32),
        NH=two((NODES, D), BF),
        NINV=two((NODES, 1), F32),
        AGG=two((NODES, D), BF),
        HS=two((HALO, D), BF),
        HR=two((HALO, D), BF),
        BS=two((HALO, D), BF),
        BR=two((HALO, D), BF),
        G=parts(lambda part: (4, 4, 2, 4)),
        RC=parts(lambda part: (4, 4, 4)),
        RA=parts(lambda part: (6,) + half_shape(part)),
        CA=parts(lambda part: (2,) + half_shape(part)),
        AB=parts(lambda part: (4, 4)),
        RB=parts(lambda part: (3, 4)),
        AD=parts(lambda part: (4,)),
        RD=parts(lambda part: (3,)),
        GZ=vm((EDGES, D), BF),
        GA=vm((EDGES, D), BF),
        GE=vm((EDGES, D), F32),
        GSR=vm((HALO_AT, D), F32),
        GV=vm((NODES, D), F32),
        GACC=vm((8, D), F32),
        WE=vm((3 * D, D), F32),
        WEO=vm((D, D), F32),
        WN=vm((2 * D, D), F32),
        WNO=vm((D, D), F32),
        load=pltpu.SemaphoreType.DMA((12,)),
        halo_send=pltpu.SemaphoreType.DMA((2, 2, 5)),
        halo_recv=pltpu.SemaphoreType.DMA((2, 2, 5)),
        rs_send=pltpu.SemaphoreType.DMA((2, 3, 13)),
        rs_recv=pltpu.SemaphoreType.DMA((2, 3, 13)),
    )


def flat_scratch():
    return jax.tree.flatten(scratch_spec())


def kernel(*refs):
    far, (eg, ng, slot, rcv, slist), (out,) = refs[:8], refs[8:13], refs[13:14]
    r = types.SimpleNamespace(**jax.tree.unflatten(flat_scratch()[1], refs[14:]))
    g = lax.axis_index(AXES[0])
    y = lax.axis_index(AXES[1])
    core = lax.rem(g, 2)
    x = lax.rem(g // 2, 4)
    z = g // 8
    place = (z, x, y)

    def peer(axis, step):
        zz = wrap(z + step, 4) if axis == 0 else z
        xx = wrap(x + step, 4) if axis == 1 else x
        yy = wrap(y + step, 4) if axis == 2 else y
        return place_id((zz * 4 + xx) * 2 + core, yy)

    def graph_peer(offset):
        return place_id(wrap(g + offset, GROUP), y)

    other_core = place_id(g + 1 - 2 * core, y)

    barrier = pltpu.get_barrier_semaphore()
    greeted = 0
    for offset in OFFSETS:
        pl.semaphore_signal(barrier, inc=1, device_id=graph_peer(offset), device_id_type=MESH)
        pl.semaphore_signal(barrier, inc=1, device_id=graph_peer(-offset), device_id_type=MESH)
        greeted += 2
    for axis in range(3):
        for step in (1, 2, 3):
            pl.semaphore_signal(barrier, inc=1, device_id=peer(axis, step), device_id_type=MESH)
            greeted += 1
    pl.semaphore_signal(barrier, inc=1, device_id=other_core, device_id_type=MESH)
    greeted += 1

    nl, el, ewi, ewo, nwi, nwo, cot, cnt = far
    pairs = [(nl, r.nl), (ewi, r.ewi, 0), (el, r.el), (ewo, r.ewo, 0), (nwi, r.nwi, 0), (nwo, r.nwo, 0)]
    pairs += [(ewi, r.ewi, 1), (ewo, r.ewo, 1), (nwi, r.nwi, 1), (nwo, r.nwo, 1), (cot, r.cot), (cnt, r.cnt)]

    def load(number):
        src, dst, *layer = pairs[number]
        if layer:
            src, dst = src.at[layer[0]], dst.at[layer[0]]
        return pltpu.make_async_copy(src, dst, r.load.at[number])

    for number in (11,) + tuple(range(11)):
        load(number).start()

    listed = jnp.concatenate(
        [slist[pl.ds(wrap(g - offset, GROUP), 1), :] for offset in OFFSETS], axis=1
    ).astype(F32)
    node_ids = iota((NODES, HALO), 0).astype(F32)
    r.LT[...] = jnp.where(node_ids == listed, 1.0, 0.0).astype(BF)

    def halo_copies(layer, way):
        src, dst = ((r.HS, r.HR), (r.BS, r.BR))[way]
        src, dst = src[layer], dst[layer]
        copies = []
        for b in reversed(range(len(OFFSETS))):
            offset = OFFSETS[b]
            rows = pl.ds(b * PEER, PEER)
            copies.append(
                pltpu.make_async_remote_copy(
                    src_ref=src.at[rows],
                    dst_ref=dst.at[rows],
                    send_sem=r.halo_send.at[layer, way, b],
                    recv_sem=r.halo_recv.at[layer, way, b],
                    device_id=graph_peer(-offset if way == 0 else offset),
                    device_id_type=MESH,
                )
            )
        return copies

    def vb(layer):
        return r.nl if layer == 0 else r.VB1

    def eb(layer):
        return r.el if layer == 0 else r.EB1

    def one_hots():
        load(11).wait()
        s = slot[...]
        within = s - NODES
        source = within // PEER
        distance = wrap(source - g, GROUP)
        block = jnp.zeros_like(s)
        for b, offset in enumerate(OFFSETS):
            block = jnp.where(distance == offset % GROUP, b, block)
        position = jnp.where(s < NODES, s, HALO_AT + block * PEER + (within - source * PEER))
        edge = iota((8, 128), 0) * 128 + iota((8, 128), 1)
        receiver = jnp.where(edge < r.cnt[0], rcv[...] + RECV_AT, -1)
        position = position.astype(F32)
        receiver = receiver.astype(F32)
        row_ids = iota((512, 128), 0).astype(F32)
        lane_ids = iota((128, 512), 1).astype(F32)
        for i in range(8):
            prow = position[i : i + 1, :]
            rrow = receiver[i : i + 1, :]
            at = slice(i * 128, (i + 1) * 128)
            for j in range(4):
                rows = slice(j * 128, (j + 1) * 128)
                row = rrow if j == 1 else prow
                r.SRT[rows, at] = jnp.where(row_ids[rows] == row, 1.0, 0.0).astype(BF)
            pcol = jnp.broadcast_to(prow, (128, 128)).T
            rcol = jnp.broadcast_to(rrow, (128, 128)).T
            for j in range(4):
                col = rcol if j == 1 else pcol
                lanes = slice(j * 128, (j + 1) * 128)
                r.SR[at, lanes] = jnp.where(lane_ids[:, lanes] == col, 1.0, 0.0).astype(BF)

    def norm(projected):
        centre = projected - jnp.mean(projected, axis=-1, keepdims=True)
        inv_std = lax.rsqrt(jnp.mean(centre * centre, axis=-1, keepdims=True) + EPSILON)
        return centre * inv_std, inv_std

    def swish(pre_act):
        sigma = 0.5 * jnp.tanh(0.5 * pre_act) + 0.5
        hidden = pre_act * sigma
        return hidden, sigma + hidden * (1.0 - sigma)

    def tile_at(t, rows):
        return pl.ds(pl.multiple_of(t * rows, rows), rows)

    def forward(layer):
        w = r.ewi.at[layer]
        wo = r.ewo.at[layer]
        nw = r.nwi.at[layer]
        nwo = r.nwo.at[layer]
        gain = eg[layer : layer + 1, :]
        ps = r.PS
        with scope("f_send"):
            if layer == 0:
                load(NL).wait()
            r.HS[layer][...] = dot_ta(r.LT[...], vb(layer)[...]).astype(BF)
            copies = halo_copies(layer, 0)
            if layer == 0:
                pl.semaphore_wait(barrier, greeted)
            for copy in copies:
                copy.start()
        with scope("f_first"):
            if layer == 0:
                one_hots()
            node = vb(layer)[...]
            load(EWI[layer]).wait()
            ps[0:NODES] = dot(node, w[D : 2 * D]).astype(BF)
            ps[RECV_AT:HALO_AT] = dot(node, w[2 * D :]).astype(BF)
            if layer == 0:
                ps[HALO_AT + HALO :] = jnp.zeros((512 - HALO_AT - HALO, D), BF)
                load(EL).wait()

            def first(t, carry):
                at = tile_at(t, FIRST)
                r.PRE[at] = dot(eb(layer)[at], w[0:D]) + dot(r.SR[at, 0:HALO_AT], ps[0:HALO_AT])
                return carry

            lax.fori_loop(0, EDGES // FIRST, first, 0)
        with scope("f_halo_wait"):
            load(EWO[layer]).wait()
            load(NWI[layer]).wait()
            load(NWO[layer]).wait()
            for copy in copies:
                copy.wait()
        with scope("f_edges"):
            ps[HALO_AT : HALO_AT + HALO] = dot(r.HR[layer][...], w[D : 2 * D]).astype(BF)

            def edges(t, carry):
                at = tile_at(t, FORE)
                pre_act = r.PRE[at] + dot(r.SR[at, HALO_AT:], ps[HALO_AT:])
                hidden, slope = swish(pre_act)
                hidden = hidden.astype(BF)
                r.H[layer][at] = hidden
                r.DA[layer][at] = slope.astype(BF)
                normed, inv_std = norm(dot(hidden, wo[...]))
                r.INV[layer][at] = inv_std
                r.N[layer][at] = normed.astype(BF)
                if layer == 0:
                    r.EB1[at] = (r.el[at].astype(F32) + normed * gain).astype(BF)
                return carry

            lax.fori_loop(0, EDGES // FORE, edges, 0, unroll=FORE_UNROLL)
        with scope("f_node"):
            agg = (dot(r.SRT[RECV_AT:HALO_AT], r.N[layer][...]) * gain).astype(BF)
            r.AGG[layer][...] = agg
            pre_act = dot(node, nw[0:D]) + dot(agg, nw[D:])
            hidden, slope = swish(pre_act)
            hidden = hidden.astype(BF)
            r.NH[layer][...] = hidden
            r.NDA[layer][...] = slope
            normed, inv_std = norm(dot(hidden, nwo[...]))
            r.NN[layer][...] = normed
            r.NINV[layer][...] = inv_std
            update = normed * ng[layer : layer + 1, :]
            if layer == 0:
                state = r.nl[...].astype(F32) + update
                r.V1[...] = state
                r.VB1[...] = state.astype(BF)
            else:
                out[0:NODES] = r.V1[...] + update

    def norm_back(grad, normed, inv_std):
        return inv_std * (
            grad
            - jnp.mean(grad, axis=-1, keepdims=True)
            - normed * jnp.mean(grad * normed, axis=-1, keepdims=True)
        )

    def fold_rows(a):
        return jnp.sum(a.reshape(a.shape[0] // 8, 8, a.shape[1]), axis=0)

    def backward_nodes(layer):
        nw = r.nwi.at[layer]
        node = vb(layer)[...]
        with scope("b_node"):
            grad = r.GV[...]
            normed = r.NN[layer][...]
            gain_sum = jnp.sum(grad * normed, axis=0, keepdims=True)
            gz = norm_back(grad * ng[layer : layer + 1, :], normed, r.NINV[layer][...]).astype(BF)
            ga = (dot_tb(gz, r.nwo[layer]) * r.NDA[layer][...]).astype(BF)
            grad_agg = dot_tb(ga, nw[D:]).astype(BF)
            r.GV[...] = grad + dot_tb(ga, nw[0:D])
            r.GACC[...] = jnp.zeros((8, D), F32)

        def weights():
            with scope("b_dwn"):
                r.WN[0:D] = dot_ta(node, ga)
                r.WN[D:] = dot_ta(r.AGG[layer][...], ga)
                r.WNO[...] = dot_ta(r.NH[layer][...], gz)

        return grad_agg, gain_sum, weights

    def backward_edges(layer, grad_agg, begin, end):
        w = r.ewi.at[layer]
        wo = r.ewo.at[layer]
        gain = eg[layer : layer + 1, :]

        def edges(t, carry):
            at = tile_at(t, BACK)
            gm = dot(r.SR[at, RECV_AT:HALO_AT], grad_agg)
            if layer == 0:
                gm = gm + r.GE[at]
            en = r.N[layer][at].astype(F32)
            r.GACC[...] += fold_rows(gm * en)
            ez = norm_back(gm * gain, en, r.INV[layer][at]).astype(BF)
            r.GZ[at] = ez
            ea = (dot_tb(ez, wo[...]) * r.DA[layer][at].astype(F32)).astype(BF)
            r.GA[at] = ea
            if layer == 1:
                r.GE[at] = dot_tb(ea, w[0:D])
            return carry

        with scope("b_edges"):
            lax.fori_loop(begin, end, edges, 0, unroll=BACK_UNROLL)

    def return_halo(layer):
        with scope("b_gsr"):
            sums = dot(r.SRT[...], r.GA[...])
            r.GSR[...] = sums[0:HALO_AT]
            r.BS[layer][...] = sums[HALO_AT : HALO_AT + HALO].astype(BF)
            copies = halo_copies(layer, 1)
            for copy in copies:
                copy.start()
        return copies

    def edge_weights(layer):
        node = vb(layer)[...]
        with scope("b_dwe"):
            r.WE[0:D] = dot_ta(eb(layer)[...], r.GA[...])
            r.WEO[...] = dot_ta(r.H[layer][...], r.GZ[...])
            to_sender = r.GSR[0:NODES].astype(BF)
            to_receiver = r.GSR[RECV_AT:HALO_AT].astype(BF)
            r.WE[D : 2 * D] = dot_ta(node, to_sender) + dot_ta(r.HR[layer][...], r.BS[layer][...])
            r.WE[2 * D :] = dot_ta(node, to_receiver)
        return jnp.sum(r.GACC[...], axis=0, keepdims=True)

    def take_halo(layer, copies):
        w = r.ewi.at[layer]
        with scope("b_halo_wait"):
            for copy in copies:
                copy.wait()
        with scope("b_tail"):
            to_sender = (r.GSR[0:NODES] + dot(r.LT[...], r.BR[layer][...])).astype(BF)
            to_receiver = r.GSR[RECV_AT:HALO_AT].astype(BF)
            total = r.GV[...] + dot_tb(to_sender, w[D : 2 * D]) + dot_tb(to_receiver, w[2 * D :])
            r.GV[...] = total
        return total

    low = iota((8, D), 0) < 4

    def each_pair(make):
        def slab(zz, carry):
            for xx in range(4):
                for cc in range(2):
                    for yy in range(2):
                        make((zz, xx, cc), 2 * yy, (zz, (xx * 2 + cc) * 2 + yy))
            return carry

        lax.fori_loop(0, 4, slab, 0)

    def pair_rows(ref, k, start, size):
        zz, inner = k
        return ref[pl.ds(pl.multiple_of(zz * 16 * size, 8) + inner * size + start, 8), :]

    def edge_slots(k):
        e0, e1, e2 = (pair_rows(r.WE, k, 8 * i, 24) for i in range(3))
        out = pltpu.roll(pair_rows(r.WEO, k, 0, 8), 4, 0)
        return (e0, jnp.where(low, e1, out)), (e2, jnp.where(low, out, e1))

    def assemble_edges(layer, gain_sum):
        def pair(where, yy, k):
            for odd, (g0, g1) in enumerate(edge_slots(k)):
                at = where + (yy + odd,)
                if layer == 1:
                    r.G[0, 0][at] = jnp.concatenate([g0, g1], axis=0).astype(BF)
                else:
                    r.G[1, 0][at] = g0[:, 0:384].astype(BF)
                    r.G[1, 1][at] = g1[:, 0:384].astype(BF)
                    r.G[1, 2][at] = jnp.concatenate([g0[:, 384:], g1[:, 384:], gains], axis=0).astype(BF)

        if layer == 0:
            lanes = [gain_sum[:, 128 * i : 128 * (i + 1)] for i in range(4)]
            gains = jnp.zeros((8, 128), F32)
            for i in range(4):
                gains = jnp.where(iota((8, 128), 0) == i, lanes[i], gains)
        with scope("asm_edges"):
            each_pair(pair)

    def assemble_nodes(layer, *gain_sums):
        row = iota((8, D), 0) % 4
        gains = jnp.zeros((8, D), F32)
        for i, gain_sum in enumerate(gain_sums):
            gains = jnp.where(row == i, gain_sum, gains)
        target = r.G[0, 1] if layer == 1 else r.G[0, 2]

        def pair(where, yy, k):
            n0, n1 = (pair_rows(r.WN, k, 8 * i, 16) for i in range(2))
            last = pair_rows(r.WNO, k, 0, 8)
            even = jnp.concatenate([n0, jnp.where(low, last, gains)], axis=0)
            odd = jnp.concatenate([n1, jnp.where(low, gains, last)], axis=0)
            target[where + (yy,)] = even.astype(BF)
            target[where + (yy + 1,)] = odd.astype(BF)

        with scope("asm_nodes"):
            each_pair(pair)

    def rs_copy(key, number, src, dst, device):
        return pltpu.make_async_remote_copy(
            src_ref=src,
            dst_ref=dst,
            send_sem=r.rs_send.at[key[0], key[1], number],
            recv_sem=r.rs_recv.at[key[0], key[1], number],
            device_id=device,
            device_id_type=MESH,
        )

    def cores(key):
        return rs_copy(key, 0, r.G[key].at[:, :, 1 - core], r.RC[key], other_core)

    def axes(key):
        first, second, third = PART_ORDER[key[1]]
        return first, second, third, second - (1 if first < second else 0)

    def cut(key, first_at, half):
        first, second, _, _ = axes(key)
        index = [slice(None)] * 3
        index[first] = first_at
        index[second] = pl.ds(2 * half, 2)
        return tuple(index)

    def ring(key, slot):
        axis = axes(key)[0]
        me = place[axis]
        way, kind = slot // 3, slot % 3
        sign = 1 - 2 * way
        if kind == 0:
            src = r.RC[key].at[cut(key, wrap(me + 2, 4), 1 - way)]
        elif kind == 1:
            src = r.RC[key].at[cut(key, wrap(me + sign, 4), way)]
        else:
            src = r.CA[key].at[way]
        return rs_copy(key, 1 + slot, src, r.RA[key].at[slot], peer(axis, sign))

    def second_copies(key):
        _, axis, _, at = axes(key)
        copies = []
        for step in (2, 1, 3):
            src = r.AB[key].at[(slice(None),) * at + (wrap(place[axis] + step, 4),)]
            copies.append(rs_copy(key, 6 + step, src, r.RB[key].at[step - 1], peer(axis, step)))
        return copies

    def third_copies(key):
        axis = axes(key)[2]
        copies = []
        for step in (2, 1, 3):
            src = r.AD[key].at[wrap(place[axis] + step, 4)]
            copies.append(rs_copy(key, 9 + step, src, r.RD[key].at[step - 1], peer(axis, step)))
        return copies

    def rs_cores(key):
        cores(key).start()

    def rs_ring(key):
        with scope("rs_ring"):
            cores(key).wait()
            mine, both = r.G[key], r.RC[key]

            def add(i, carry):
                both[i] = both[i] + mine[i, :, core]
                return carry

            lax.fori_loop(0, 4, add, 0)
            for slot in (0, 3, 1, 4):
                ring(key, slot).start()

    def rs_sums(key):
        with scope("rs_sums"):
            me = place[axes(key)[0]]
            for way, sign in ((0, 1), (1, -1)):
                ring(key, 3 * way).wait()
                own = r.RC[key][cut(key, wrap(me + sign, 4), 1 - way)]
                r.CA[key][way] = own + r.RA[key][3 * way]
                ring(key, 3 * way + 2).start()

    def rs_second(key):
        with scope("rs_second"):
            first, axis, _, at = axes(key)
            for slot in (1, 4, 2, 5):
                ring(key, slot).wait()
            got = r.RA[key]
            for half in range(2):
                near, summed = (1, 5) if half == 0 else (4, 2)
                total = r.RC[key][cut(key, place[first], half)].astype(F32)
                total = total + got[near].astype(F32) + got[summed].astype(F32)
                index = (slice(None),) * at + (slice(2 * half, 2 * half + 2),)
                r.AB[key][index] = total.astype(BF)
            for copy in second_copies(key):
                copy.start()

    def rs_third(key):
        with scope("rs_third"):
            _, axis, _, at = axes(key)
            for copy in second_copies(key):
                copy.wait()
            total = r.AB[key][(slice(None),) * at + (place[axis],)].astype(F32)
            for i in range(3):
                total = total + r.RB[key][i].astype(F32)
            r.AD[key][...] = total.astype(BF)
            for copy in third_copies(key):
                copy.start()

    def rs_finish(key):
        with scope("rs_finish"):
            for copy in third_copies(key):
                copy.wait()
            total = r.AD[key][place[axes(key)[2]]].astype(F32)
            for i in range(3):
                total = total + r.RD[key][i].astype(F32)
            stream, part = key
            if stream == 0:
                out[SUMS_AT + 16 * part : SUMS_AT + 16 * part + 16] = total
            elif part < 2:
                out[SUMS_AT + 48 + 8 * part : SUMS_AT + 56 + 8 * part, 0:384] = total
            else:
                for i in range(2):
                    out[SUMS_AT + 48 + 8 * i : SUMS_AT + 56 + 8 * i, 384:] = total[8 * i : 8 * i + 8]
                out[SUMS_AT + 64 :, 0:128] = total[16:24]

    early = ((0, 0), (0, 1), (0, 2))
    late = ((1, 0), (1, 1), (1, 2))

    def each(call, keys):
        for key in keys:
            call(key)

    forward(0)
    forward(1)
    load(COT).wait()
    r.GV[...] = r.cot[...].astype(F32)
    count = EDGES // BACK

    grad_agg, node_gain, node_weights = backward_nodes(1)
    backward_edges(1, grad_agg, 0, count)
    copies = return_halo(1)
    edge_gain = edge_weights(1)
    assemble_edges(1, None)
    rs_cores((0, 0))
    node_weights()
    assemble_nodes(1, edge_gain, node_gain)
    rs_cores((0, 1))
    take_halo(1, copies)
    rs_ring((0, 0))

    grad_agg, node_gain, node_weights = backward_nodes(0)
    node_weights()
    assemble_nodes(0, node_gain)
    rs_cores((0, 2))
    rs_ring((0, 1))
    backward_edges(0, grad_agg, 0, count)
    rs_ring((0, 2))
    copies = return_halo(0)
    rs_sums((0, 0))
    edge_gain = edge_weights(0)
    rs_sums((0, 1))
    assemble_edges(0, edge_gain)
    each(rs_cores, late)
    rs_sums((0, 2))
    each(rs_ring, late)
    out[NODES : 2 * NODES] = take_halo(0, copies)
    rs_second((0, 0))
    each(rs_sums, late)
    rs_second((0, 1))
    rs_second((0, 2))
    rs_third((0, 0))
    each(rs_second, late)
    rs_third((0, 1))
    rs_third((0, 2))
    each(rs_third, late)
    each(rs_finish, early)
    each(rs_finish, late)


def finish_kernel(sums, o_node, o_grad, o_ei, o_eo, o_ni, o_no, o_eg, o_ng):
    y = lax.axis_index(AXES[1])
    column = (lax.axis_index(AXES[0]) * SAMPLES + y) * 4
    is_even = lax.rem(y, 2) == 0
    o_node[...] = sums[0:NODES]
    o_grad[...] = sums[NODES : 2 * NODES]

    def edge_rows(layer, g0, g1):
        even = jnp.concatenate([g0, g1[0:4]], axis=0)
        odd = jnp.concatenate([g1[4:8], g0], axis=0)
        o_ei[:, layer] = jnp.where(is_even, even, odd)
        o_eo[layer] = jnp.where(is_even, g1[4:8], g1[0:4])

    def node_rows(layer, total):
        o_ni[layer] = total[0:8]
        last = total[8:16]
        o_no[layer] = jnp.where(is_even, last[0:4], last[4:8])
        return jnp.where(is_even, last[4:8], last[0:4])

    def four(row):
        lane = iota((1, D), 1)
        at = iota((1, 4), 1)
        picked = jnp.zeros((1, 4), F32)
        for i in range(4):
            value = jnp.sum(jnp.where(lane == column + i, row, 0.0), axis=1, keepdims=True)
            picked = jnp.where(at == i, value, picked)
        return picked

    def rows(start, size):
        return sums[SUMS_AT + start : SUMS_AT + start + size]

    edge_rows(1, rows(0, 8), rows(8, 8))
    edge_rows(0, rows(48, 8), rows(56, 8))
    gains = node_rows(1, rows(16, 16))
    o_eg[1:2] = four(gains[0:1])
    o_ng[1:2] = four(gains[1:2])
    o_ng[0:1] = four(node_rows(0, rows(32, 16))[0:1])
    last = rows(64, 8)
    o_eg[0:1] = four(jnp.concatenate([last[i : i + 1, 0:128] for i in range(4)], axis=1))


def body(*args):
    (node_latent, edge_latent, node_cotangent, ewi, ewo, nwi, nwo, *gains, edge_slot, edge_receiver, send_list, edge_count) = args
    vmem = pl.BlockSpec(memory_space=pltpu.VMEM)
    far = pl.BlockSpec(memory_space=pl.ANY)
    results = pl.pallas_call(
        kernel,
        out_shape=jax.ShapeDtypeStruct((SUMS_AT + 72, D), F32),
        in_specs=[far] * 8 + [vmem] * 5,
        out_specs=vmem,
        scratch_shapes=flat_scratch()[0],
        compiler_params=pltpu.CompilerParams(
            collective_id=0, has_side_effects=True, vmem_limit_bytes=VMEM_LIMIT
        ),
        cost_estimate=pl.CostEstimate(flops=10**10, bytes_accessed=10**7, transcendentals=10**6),
    )(
        node_latent[0],
        edge_latent[0],
        ewi,
        ewo,
        nwi,
        nwo,
        node_cotangent[0],
        edge_count,
        *gains,
        edge_slot.reshape(8, 128),
        edge_receiver.reshape(8, 128),
        send_list,
    )
    outs = (
        (NODES, D),
        (NODES, D),
        (12, 2, D),
        (2, 4, D),
        (2, 8, D),
        (2, 4, D),
        (2, 4),
        (2, 4),
    )
    results = pl.pallas_call(
        finish_kernel,
        out_shape=tuple(jax.ShapeDtypeStruct(shape, F32) for shape in outs),
        in_specs=[vmem],
        out_specs=tuple([vmem] * 8),
        compiler_params=pltpu.CompilerParams(vmem_limit_bytes=VMEM_LIMIT),
    )(results)
    return (results[0][None], results[1][None], jnp.transpose(results[2], (1, 0, 2))) + tuple(results[3:])


def solution(mesh):
    nodes = P(AXES[1], AXES[0], None)
    graph = P(AXES[0])
    in_specs = (nodes, nodes, nodes) + (P(),) * 6 + (graph, graph, P(AXES[0], None), graph)
    rows = P(None, AXES, None)
    out_specs = (nodes, nodes) + (rows,) * 4 + (P(None, AXES),) * 2
    return jax.shard_map(body, mesh=mesh, in_specs=in_specs, out_specs=out_specs, check_vma=False)
```

```python
import types

import jax
import jax.numpy as jnp
from jax import lax
from jax.experimental import pallas as pl
from jax.experimental.pallas import tpu as pltpu
from jax.sharding import PartitionSpec as P

HOPS = 2
EPSILON = 1e-05
BF = jnp.bfloat16
F32 = jnp.float32
D = 512
NODES = 128
EDGES = 1024
PEER = 32
GROUP = 32
SAMPLES = 4
VMEM_LIMIT = 62 * 1024 * 1024
OFFSETS = tuple(o for o in range(-HOPS, HOPS + 1) if o != 0) + (GROUP // 2,)
HALO = len(OFFSETS) * PEER
RECV_AT = NODES
HALO_AT = 2 * NODES
SUMS_AT = 2 * NODES
FIRST, FORE, BACK = 1024, 1024, 1024
FORE_UNROLL, BACK_UNROLL = 1, 1
MESH = pl.DeviceIdType.MESH
STREAM_TILES = (
    ((16, 384), (16, 384), (32, 128)),
    ((8, 384), (8, 384), (16, 128)),
    ((8, 384), (8, 384), (24, 128)),
)
PART_ORDER = ((1, 2, 0), (2, 0, 1), (0, 1, 2))
AXES = ("graph", "batch")
scope = jax.named_scope


def dot(a, b):
    return jnp.dot(a, b, preferred_element_type=F32)


def dot_tb(a, b):
    return lax.dot_general(a, b, (((1,), (1,)), ((), ())), preferred_element_type=F32)


def dot_ta(a, b):
    return lax.dot_general(a, b, (((0,), (0,)), ((), ())), preferred_element_type=F32)


def place_id(graph, batch):
    return dict(zip(AXES, (graph, batch)))


def wrap(value, size):
    return lax.rem(value + 2 * size, size)


def iota(shape, dim):
    return lax.broadcasted_iota(jnp.int32, shape, dim)


def half_shape(part):
    first, second, _ = PART_ORDER[part]
    shape = [4, 4, 4]
    shape[second] = 2
    del shape[first]
    return tuple(shape)


NL, EWI, EL, EWO, NWI, NWO, COT = 0, (1, 6), 2, (3, 7), (4, 8), (5, 9), 10


def scratch_spec():
    vm = pltpu.VMEM

    def two(shape, dtype):
        return [vm(shape, dtype), vm(shape, dtype)]

    def parts(shape):
        keys = [(stream, part) for stream in range(3) for part in range(3)]
        return {key: vm(shape(key[1]) + STREAM_TILES[key[0]][key[1]], BF) for key in keys}

    return dict(
        nl=vm((NODES, D), BF),
        el=vm((EDGES, D), BF),
        ewi=vm((2, 3 * D, D), BF),
        ewo=vm((2, D, D), BF),
        nwi=vm((2, 2 * D, D), BF),
        nwo=vm((2, D, D), BF),
        cot=vm((NODES, D), BF),
        cnt=pltpu.SMEM((1,), jnp.int32),
        small=[
            vm((2, D), F32),
            vm((2, D), F32),
            vm((8, 128), jnp.int32),
            vm((8, 128), jnp.int32),
            vm((GROUP, PEER), jnp.int32),
        ],
        SR=vm((EDGES, 512), BF),
        SRT=vm((512, EDGES), BF),
        LT=vm((NODES, HALO), BF),
        PS=vm((512, D), BF),
        PRE=vm((EDGES, D), F32),
        EB1=vm((EDGES, D), BF),
        VB1=vm((NODES, D), BF),
        V1=vm((NODES, D), F32),
        NPRE=vm((NODES, D), F32),
        N=two((EDGES, D), BF),
        DA=two((EDGES, D), BF),
        H=two((EDGES, D), BF),
        INV=two((EDGES, 1), F32),
        NN=two((NODES, D), F32),
        NDA=two((NODES, D), F32),
        NH=two((NODES, D), BF),
        NINV=two((NODES, 1), F32),
        AGG=two((NODES, D), BF),
        HS=two((HALO, D), BF),
        HR=two((HALO, D), BF),
        BS=two((HALO, D), BF),
        BR=two((HALO, D), BF),
        G=parts(lambda part: (4, 4, 2, 4)),
        RC=parts(lambda part: (4, 4, 4)),
        RA=parts(lambda part: (6,) + half_shape(part)),
        CA=parts(lambda part: (2,) + half_shape(part)),
        AB=parts(lambda part: (4, 4)),
        RB=parts(lambda part: (3, 4)),
        AD=parts(lambda part: (4,)),
        RD=parts(lambda part: (3,)),
        GZ=vm((EDGES, D), BF),
        GA=vm((EDGES, D), BF),
        GSR=vm((HALO_AT, D), F32),
        GV=vm((NODES, D), F32),
        GACC=vm((8, D), F32),
        WE=vm((3 * D, D), F32),
        WEO=vm((D, D), F32),
        WN=vm((2 * D, D), F32),
        WNO=vm((D, D), F32),
        OUT=vm((SUMS_AT + 72, D), F32),
        store=pltpu.SemaphoreType.DMA((3,)),
        load=pltpu.SemaphoreType.DMA((17,)),
        halo_send=pltpu.SemaphoreType.DMA((2, 2, 5)),
        halo_recv=pltpu.SemaphoreType.DMA((2, 2, 5)),
        rs_send=pltpu.SemaphoreType.DMA((3, 3, 13)),
        rs_recv=pltpu.SemaphoreType.DMA((3, 3, 13)),
    )


def flat_scratch():
    return jax.tree.flatten(scratch_spec())


def kernel(*refs):
    far, out = refs[:13], refs[13]
    r = types.SimpleNamespace(**jax.tree.unflatten(flat_scratch()[1], refs[14:]))
    g = lax.axis_index(AXES[0])
    y = lax.axis_index(AXES[1])
    core = lax.rem(g, 2)
    x = lax.rem(g // 2, 4)
    z = g // 8
    place = (z, x, y)

    def peer(axis, step):
        zz = wrap(z + step, 4) if axis == 0 else z
        xx = wrap(x + step, 4) if axis == 1 else x
        yy = wrap(y + step, 4) if axis == 2 else y
        return place_id((zz * 4 + xx) * 2 + core, yy)

    def graph_peer(offset):
        return place_id(wrap(g + offset, GROUP), y)

    other_core = place_id(g + 1 - 2 * core, y)

    barrier = pltpu.get_barrier_semaphore()
    greeted = 0
    for offset in OFFSETS:
        pl.semaphore_signal(barrier, inc=1, device_id=graph_peer(offset), device_id_type=MESH)
        pl.semaphore_signal(barrier, inc=1, device_id=graph_peer(-offset), device_id_type=MESH)
        greeted += 2
    for axis in range(3):
        for step in (1, 2, 3):
            pl.semaphore_signal(barrier, inc=1, device_id=peer(axis, step), device_id_type=MESH)
            greeted += 1
    pl.semaphore_signal(barrier, inc=1, device_id=other_core, device_id_type=MESH)
    greeted += 1

    nl, el, ewi, ewo, nwi, nwo, cot, cnt, *small = far
    pairs = [(nl, r.nl), (ewi, r.ewi, 0), (el, r.el), (ewo, r.ewo, 0), (nwi, r.nwi, 0), (nwo, r.nwo, 0)]
    pairs += [(ewi, r.ewi, 1), (ewo, r.ewo, 1), (nwi, r.nwi, 1), (nwo, r.nwo, 1), (cot, r.cot), (cnt, r.cnt)]
    eg, ng, slot, rcv, slist = r.small
    pairs += list(zip(small, r.small))

    def load(number):
        src, dst, *layer = pairs[number]
        if layer:
            src, dst = src.at[layer[0]], dst.at[layer[0]]
        return pltpu.make_async_copy(src, dst, r.load.at[number])

    for number in (16, 0, 14, 15, 11) + tuple(range(1, 11)) + (12, 13):
        load(number).start()

    load(16).wait()
    listed = jnp.concatenate(
        [slist[pl.ds(wrap(g - offset, GROUP), 1), :] for offset in OFFSETS], axis=1
    ).astype(F32)
    node_ids = iota((NODES, HALO), 0).astype(F32)
    r.LT[...] = jnp.where(node_ids == listed, 1.0, 0.0).astype(BF)

    def halo_copies(layer, way):
        src, dst = ((r.HS, r.HR), (r.BS, r.BR))[way]
        src, dst = src[layer], dst[layer]
        copies = []
        for b in reversed(range(len(OFFSETS))):
            offset = OFFSETS[b]
            rows = pl.ds(b * PEER, PEER)
            copies.append(
                pltpu.make_async_remote_copy(
                    src_ref=src.at[rows],
                    dst_ref=dst.at[rows],
                    send_sem=r.halo_send.at[layer, way, b],
                    recv_sem=r.halo_recv.at[layer, way, b],
                    device_id=graph_peer(-offset if way == 0 else offset),
                    device_id_type=MESH,
                )
            )
        return copies

    def vb(layer):
        return r.nl if layer == 0 else r.VB1

    def eb(layer):
        return r.el if layer == 0 else r.EB1

    def one_hots():
        for number in (11, 14, 15):
            load(number).wait()
        s = slot[...]
        within = s - NODES
        source = within // PEER
        distance = wrap(source - g, GROUP)
        block = jnp.zeros_like(s)
        for b, offset in enumerate(OFFSETS):
            block = jnp.where(distance == offset % GROUP, b, block)
        position = jnp.where(s < NODES, s, HALO_AT + block * PEER + (within - source * PEER))
        edge = iota((8, 128), 0) * 128 + iota((8, 128), 1)
        receiver = jnp.where(edge < r.cnt[0], rcv[...] + RECV_AT, -1)
        position = position.astype(F32)
        receiver = receiver.astype(F32)
        row_ids = iota((512, 128), 0).astype(F32)
        lane_ids = iota((128, 512), 1).astype(F32)
        for i in range(8):
            prow = position[i : i + 1, :]
            rrow = receiver[i : i + 1, :]
            at = slice(i * 128, (i + 1) * 128)
            for j in range(4):
                rows = slice(j * 128, (j + 1) * 128)
                row = rrow if j == 1 else prow
                r.SRT[rows, at] = jnp.where(row_ids[rows] == row, 1.0, 0.0).astype(BF)
            pcol = jnp.broadcast_to(prow, (128, 128)).T
            rcol = jnp.broadcast_to(rrow, (128, 128)).T
            for j in range(4):
                col = rcol if j == 1 else pcol
                lanes = slice(j * 128, (j + 1) * 128)
                r.SR[at, lanes] = jnp.where(lane_ids[:, lanes] == col, 1.0, 0.0).astype(BF)

    def norm(projected):
        centre = projected - jnp.mean(projected, axis=-1, keepdims=True)
        inv_std = lax.rsqrt(jnp.mean(centre * centre, axis=-1, keepdims=True) + EPSILON)
        return centre * inv_std, inv_std

    def swish(pre_act):
        sigma = 0.5 * jnp.tanh(0.5 * pre_act) + 0.5
        hidden = pre_act * sigma
        return hidden, sigma + hidden * (1.0 - sigma)

    def tile_at(t, rows):
        return pl.ds(pl.multiple_of(t * rows, rows), rows)

    def forward(layer):
        w = r.ewi.at[layer]
        wo = r.ewo.at[layer]
        nw = r.nwi.at[layer]
        nwo = r.nwo.at[layer]
        ps = r.PS
        with scope("f_send"):
            if layer == 0:
                load(NL).wait()
            r.HS[layer][...] = dot_ta(r.LT[...], vb(layer)[...]).astype(BF)
            copies = halo_copies(layer, 0)
            if layer == 0:
                pl.semaphore_wait(barrier, greeted)
            for copy in copies:
                copy.start()
        with scope("f_first"):
            if layer == 0:
                one_hots()
            node = vb(layer)[...]
            load(EWI[layer]).wait()
            ps[0:NODES] = dot(node, w[D : 2 * D]).astype(BF)
            ps[RECV_AT:HALO_AT] = dot(node, w[2 * D :]).astype(BF)
            if layer == 0:
                ps[HALO_AT + HALO :] = jnp.zeros((512 - HALO_AT - HALO, D), BF)
                load(EL).wait()

            def first(t, carry):
                at = tile_at(t, FIRST)
                r.PRE[at] = dot(eb(layer)[at], w[0:D]) + dot(r.SR[at, 0:HALO_AT], ps[0:HALO_AT])
                return carry

            lax.fori_loop(0, EDGES // FIRST, first, 0)
            load(NWI[layer]).wait()
            r.NPRE[...] = dot(node, nw[0:D])
        with scope("f_halo_wait"):
            load(EWO[layer]).wait()
            load(NWO[layer]).wait()
            for copy in copies:
                copy.wait()
        with scope("f_edges"):
            if layer == 0:
                load(12).wait()
                load(13).wait()
            gain = eg[layer : layer + 1, :]
            ps[HALO_AT : HALO_AT + HALO] = dot(r.HR[layer][...], w[D : 2 * D]).astype(BF)

            def edges(t, carry):
                at = tile_at(t, FORE)
                pre_act = r.PRE[at] + dot(r.SR[at, HALO_AT:], ps[HALO_AT:])
                hidden, slope = swish(pre_act)
                hidden = hidden.astype(BF)
                r.H[layer][at] = hidden
                r.DA[layer][at] = slope.astype(BF)
                normed, inv_std = norm(dot(hidden, wo[...]))
                r.INV[layer][at] = inv_std
                r.N[layer][at] = normed.astype(BF)
                if layer == 0:
                    r.EB1[at] = (r.el[at].astype(F32) + normed * gain).astype(BF)
                return carry

            lax.fori_loop(0, EDGES // FORE, edges, 0, unroll=FORE_UNROLL)
        with scope("f_node"):
            agg = (dot(r.SRT[RECV_AT:HALO_AT], r.N[layer][...]) * gain).astype(BF)
            r.AGG[layer][...] = agg
            pre_act = r.NPRE[...] + dot(agg, nw[D:])
            hidden, slope = swish(pre_act)
            hidden = hidden.astype(BF)
            r.NH[layer][...] = hidden
            r.NDA[layer][...] = slope
            normed, inv_std = norm(dot(hidden, nwo[...]))
            r.NN[layer][...] = normed
            r.NINV[layer][...] = inv_std
            update = normed * ng[layer : layer + 1, :]
            if layer == 0:
                state = r.nl[...].astype(F32) + update
                r.V1[...] = state
                r.VB1[...] = state.astype(BF)
            else:
                r.OUT[0:NODES] = r.V1[...] + update

    def norm_back(grad, normed, inv_std):
        return inv_std * (
            grad
            - jnp.mean(grad, axis=-1, keepdims=True)
            - normed * jnp.mean(grad * normed, axis=-1, keepdims=True)
        )

    def fold_rows(a):
        return jnp.sum(a.reshape(a.shape[0] // 8, 8, a.shape[1]), axis=0)

    def backward_nodes(layer):
        nw = r.nwi.at[layer]
        node = vb(layer)[...]
        with scope("b_node"):
            grad = r.GV[...]
            normed = r.NN[layer][...]
            gain_sum = jnp.sum(grad * normed, axis=0, keepdims=True)
            gz = norm_back(grad * ng[layer : layer + 1, :], normed, r.NINV[layer][...]).astype(BF)
            ga = (dot_tb(gz, r.nwo[layer]) * r.NDA[layer][...]).astype(BF)
            grad_agg = dot_tb(ga, nw[D:]).astype(BF)
            r.GACC[...] = jnp.zeros((8, D), F32)

        def weights():
            with scope("b_dwn"):
                r.WN[0:D] = dot_ta(node, ga)
                r.WN[D:] = dot_ta(r.AGG[layer][...], ga)
                r.WNO[...] = dot_ta(r.NH[layer][...], gz)
                r.GV[...] = r.GV[...] + dot_tb(ga, nw[0:D])

        return grad_agg, gain_sum, weights

    def backward_edges(layer, grad_agg):
        wo = r.ewo.at[layer]
        gain = eg[layer : layer + 1, :]

        def edges(t, carry):
            at = tile_at(t, BACK)
            gm = dot(r.SR[at, RECV_AT:HALO_AT], grad_agg)
            if layer == 0:
                gm = gm + r.PRE[at]
            en = r.N[layer][at].astype(F32)
            r.GACC[...] += fold_rows(gm * en)
            ez = norm_back(gm * gain, en, r.INV[layer][at]).astype(BF)
            r.GZ[at] = ez
            ea = (dot_tb(ez, wo[...]) * r.DA[layer][at].astype(F32)).astype(BF)
            r.GA[at] = ea
            return carry

        with scope("b_edges"):
            lax.fori_loop(0, EDGES // BACK, edges, 0, unroll=BACK_UNROLL)

    def return_halo(layer):
        with scope("b_gsr"):
            sums = dot(r.SRT[...], r.GA[...])
            r.GSR[...] = sums[0:HALO_AT]
            r.BS[layer][...] = sums[HALO_AT : HALO_AT + HALO].astype(BF)
            copies = halo_copies(layer, 1)
            for copy in copies:
                copy.start()
        return copies

    def edge_weights(layer):
        node = vb(layer)[...]
        with scope("b_dwe"):
            r.WE[0:D] = dot_ta(eb(layer)[...], r.GA[...])
            r.WEO[...] = dot_ta(r.H[layer][...], r.GZ[...])
            to_sender = r.GSR[0:NODES].astype(BF)
            to_receiver = r.GSR[RECV_AT:HALO_AT].astype(BF)
            r.WE[D : 2 * D] = dot_ta(node, to_sender) + dot_ta(r.HR[layer][...], r.BS[layer][...])
            r.WE[2 * D :] = dot_ta(node, to_receiver)
        return jnp.sum(r.GACC[...], axis=0, keepdims=True)

    def edge_inputs(layer):
        with scope("b_inputs"):
            to_receiver = r.GSR[RECV_AT:HALO_AT].astype(BF)
            r.GV[...] = r.GV[...] + dot_tb(to_receiver, r.ewi[layer, 2 * D :])
            if layer == 1:
                r.PRE[...] = dot_tb(r.GA[...], r.ewi[layer, 0:D])

    def take_halo(layer, copies):
        w = r.ewi.at[layer]
        with scope("b_halo_wait"):
            for copy in copies:
                copy.wait()
        with scope("b_tail"):
            to_sender = (r.GSR[0:NODES] + dot(r.LT[...], r.BR[layer][...])).astype(BF)
            total = r.GV[...] + dot_tb(to_sender, w[D : 2 * D])
            r.GV[...] = total
        return total

    low = iota((8, D), 0) < 4

    def each_pair(make):
        def slab(zz, carry):
            for xx in range(4):
                for cc in range(2):
                    for yy in range(2):
                        make((zz, xx, cc), 2 * yy, (zz, (xx * 2 + cc) * 2 + yy))
            return carry

        lax.fori_loop(0, 4, slab, 0)

    def pair_rows(ref, k, start, size):
        zz, inner = k
        return ref[pl.ds(pl.multiple_of(zz * 16 * size, 8) + inner * size + start, 8), :]

    def edge_slots(k):
        e0, e1, e2 = (pair_rows(r.WE, k, 8 * i, 24) for i in range(3))
        out = pltpu.roll(pair_rows(r.WEO, k, 0, 8), 4, 0)
        return (e0, jnp.where(low, e1, out)), (e2, jnp.where(low, out, e1))

    def assemble_edges(layer, gain_sum):
        def pair(where, yy, k):
            for odd, (g0, g1) in enumerate(edge_slots(k)):
                at = where + (yy + odd,)
                if layer == 1:
                    both = jnp.concatenate([g0, g1], axis=0).astype(BF)
                    r.G[0, 0][at] = both[:, 0:384]
                    r.G[0, 2][at + (slice(0, 16),)] = both[:, 384:]
                else:
                    r.G[2, 0][at] = g0[:, 0:384].astype(BF)
                    r.G[2, 1][at] = g1[:, 0:384].astype(BF)
                    r.G[2, 2][at] = jnp.concatenate([g0[:, 384:], g1[:, 384:], gains], axis=0).astype(BF)

        if layer == 0:
            lanes = [gain_sum[:, 128 * i : 128 * (i + 1)] for i in range(4)]
            gains = jnp.zeros((8, 128), F32)
            for i in range(4):
                gains = jnp.where(iota((8, 128), 0) == i, lanes[i], gains)
        with scope("asm_edges"):
            each_pair(pair)

    def assemble_nodes(layer, *gain_sums):
        row = iota((8, D), 0) % 4
        gains = jnp.zeros((8, D), F32)
        for i, gain_sum in enumerate(gain_sums):
            gains = jnp.where(row == i, gain_sum, gains)
        def pair(where, yy, k):
            n0, n1 = (pair_rows(r.WN, k, 8 * i, 16) for i in range(2))
            last = pair_rows(r.WNO, k, 0, 8)
            slots = ((n0, jnp.where(low, last, gains)), (n1, jnp.where(low, gains, last)))
            for odd, (g2, g3) in enumerate(slots):
                at = where + (yy + odd,)
                if layer == 1:
                    both = jnp.concatenate([g2, g3], axis=0).astype(BF)
                    r.G[0, 1][at] = both[:, 0:384]
                    r.G[0, 2][at + (slice(16, 32),)] = both[:, 384:]
                else:
                    r.G[1, 0][at] = g2[:, 0:384].astype(BF)
                    r.G[1, 1][at] = g3[:, 0:384].astype(BF)
                    r.G[1, 2][at] = jnp.concatenate([g2[:, 384:], g3[:, 384:]], axis=0).astype(BF)

        with scope("asm_nodes"):
            each_pair(pair)

    def rs_copy(key, number, src, dst, device):
        return pltpu.make_async_remote_copy(
            src_ref=src,
            dst_ref=dst,
            send_sem=r.rs_send.at[key[0], key[1], number],
            recv_sem=r.rs_recv.at[key[0], key[1], number],
            device_id=device,
            device_id_type=MESH,
        )

    def cores(key):
        return rs_copy(key, 0, r.G[key].at[:, :, 1 - core], r.RC[key], other_core)

    def axes(key):
        first, second, third = PART_ORDER[key[1]]
        return first, second, third, second - (1 if first < second else 0)

    def cut(key, first_at, half):
        first, second, _, _ = axes(key)
        index = [slice(None)] * 3
        index[first] = first_at
        index[second] = pl.ds(2 * half, 2)
        return tuple(index)

    def ring(key, slot):
        axis = axes(key)[0]
        me = place[axis]
        way, kind = slot // 3, slot % 3
        sign = 1 - 2 * way
        if kind == 0:
            src = r.RC[key].at[cut(key, wrap(me + 2, 4), 1 - way)]
        elif kind == 1:
            src = r.RC[key].at[cut(key, wrap(me + sign, 4), way)]
        else:
            src = r.CA[key].at[way]
        return rs_copy(key, 1 + slot, src, r.RA[key].at[slot], peer(axis, sign))

    def second_copies(key):
        _, axis, _, at = axes(key)
        copies = []
        for step in (2, 1, 3):
            src = r.AB[key].at[(slice(None),) * at + (wrap(place[axis] + step, 4),)]
            copies.append(rs_copy(key, 6 + step, src, r.RB[key].at[step - 1], peer(axis, step)))
        return copies

    def third_copies(key):
        axis = axes(key)[2]
        copies = []
        for step in (2, 1, 3):
            src = r.AD[key].at[wrap(place[axis] + step, 4)]
            copies.append(rs_copy(key, 9 + step, src, r.RD[key].at[step - 1], peer(axis, step)))
        return copies

    def rs_cores(key):
        cores(key).start()

    def rs_ring(key):
        with scope("rs_ring"):
            cores(key).wait()
            mine, both = r.G[key], r.RC[key]

            def add(i, carry):
                both[i] = both[i] + mine[i, :, core]
                return carry

            lax.fori_loop(0, 4, add, 0)
            for slot in (0, 3, 1, 4):
                ring(key, slot).start()

    def rs_sums(key):
        with scope("rs_sums"):
            me = place[axes(key)[0]]
            for way, sign in ((0, 1), (1, -1)):
                ring(key, 3 * way).wait()
                own = r.RC[key][cut(key, wrap(me + sign, 4), 1 - way)]
                r.CA[key][way] = own + r.RA[key][3 * way]
                ring(key, 3 * way + 2).start()

    def rs_second(key):
        with scope("rs_second"):
            first, axis, _, at = axes(key)
            for slot in (1, 4, 2, 5):
                ring(key, slot).wait()
            got = r.RA[key]
            for half in range(2):
                near, summed = (1, 5) if half == 0 else (4, 2)
                total = r.RC[key][cut(key, place[first], half)].astype(F32)
                total = total + got[near].astype(F32) + got[summed].astype(F32)
                index = (slice(None),) * at + (slice(2 * half, 2 * half + 2),)
                r.AB[key][index] = total.astype(BF)
            for copy in second_copies(key):
                copy.start()

    def rs_third(key):
        with scope("rs_third"):
            _, axis, _, at = axes(key)
            for copy in second_copies(key):
                copy.wait()
            total = r.AB[key][(slice(None),) * at + (place[axis],)].astype(F32)
            for i in range(3):
                total = total + r.RB[key][i].astype(F32)
            r.AD[key][...] = total.astype(BF)
            for copy in third_copies(key):
                copy.start()

    def rs_finish(key):
        with scope("rs_finish"):
            for copy in third_copies(key):
                copy.wait()
            total = r.AD[key][place[axes(key)[2]]].astype(F32)
            for i in range(3):
                total = total + r.RD[key][i].astype(F32)
            stream, part = key
            start = SUMS_AT + (0, 32, 48)[stream]
            rows = 16 if stream == 0 else 8
            if part < 2:
                r.OUT[start + rows * part : start + rows * part + rows, 0:384] = total
            else:
                r.OUT[start : start + 2 * rows, 384:] = total[0 : 2 * rows]
            if key == (2, 2):
                r.OUT[SUMS_AT + 64 :, 0:128] = total[16:24]

    def store(number):
        rows = pl.ds((0, NODES, SUMS_AT)[number], (NODES, NODES, 72)[number])
        return pltpu.make_async_copy(r.OUT.at[rows], out.at[rows], r.store.at[number])

    def each(call, stream, *parts):
        for part in parts or range(3):
            call((stream, part))

    forward(0)
    forward(1)
    store(0).start()
    load(COT).wait()
    r.GV[...] = r.cot[...].astype(F32)

    grad_agg, node_gain, node_weights = backward_nodes(1)
    backward_edges(1, grad_agg)
    copies = return_halo(1)
    edge_gain = edge_weights(1)
    assemble_edges(1, None)
    each(rs_cores, 0, 0)
    edge_inputs(1)
    node_weights()
    assemble_nodes(1, edge_gain, node_gain)
    each(rs_cores, 0, 1, 2)
    take_halo(1, copies)
    each(rs_ring, 0, 0)

    grad_agg, node_gain, node_weights = backward_nodes(0)
    node_weights()
    assemble_nodes(0, node_gain)
    each(rs_cores, 1)
    each(rs_ring, 0, 1, 2)
    backward_edges(0, grad_agg)
    copies = return_halo(0)
    each(rs_ring, 1)
    each(rs_sums, 0, 0)
    edge_gain = edge_weights(0)
    assemble_edges(0, edge_gain)
    each(rs_cores, 2)
    each(rs_sums, 0, 1, 2)
    edge_inputs(0)
    each(rs_ring, 2)
    each(rs_sums, 1)
    each(rs_second, 0)
    each(rs_sums, 2)
    each(rs_second, 1)
    r.OUT[NODES : 2 * NODES] = take_halo(0, copies)
    store(1).start()
    each(rs_third, 0)
    each(rs_second, 2)
    each(rs_third, 1)
    each(rs_third, 2)
    for stream in range(3):
        each(rs_finish, stream)
    store(2).start()
    for number in range(3):
        store(number).wait()


def finish_kernel(sums, o_node, o_grad, o_ei, o_eo, o_ni, o_no, o_eg, o_ng):
    y = lax.axis_index(AXES[1])
    column = (lax.axis_index(AXES[0]) * SAMPLES + y) * 4
    is_even = lax.rem(y, 2) == 0
    o_node[...] = sums[0:NODES]
    o_grad[...] = sums[NODES : 2 * NODES]

    def edge_rows(layer, g0, g1):
        even = jnp.concatenate([g0, g1[0:4]], axis=0)
        odd = jnp.concatenate([g1[4:8], g0], axis=0)
        o_ei[:, layer] = jnp.where(is_even, even, odd)
        o_eo[layer] = jnp.where(is_even, g1[4:8], g1[0:4])

    def node_rows(layer, total):
        o_ni[layer] = total[0:8]
        last = total[8:16]
        o_no[layer] = jnp.where(is_even, last[0:4], last[4:8])
        return jnp.where(is_even, last[4:8], last[0:4])

    def four(row):
        lane = iota((1, D), 1)
        at = iota((1, 4), 1)
        picked = jnp.zeros((1, 4), F32)
        for i in range(4):
            value = jnp.sum(jnp.where(lane == column + i, row, 0.0), axis=1, keepdims=True)
            picked = jnp.where(at == i, value, picked)
        return picked

    def rows(start, size):
        return sums[SUMS_AT + start : SUMS_AT + start + size]

    edge_rows(1, rows(0, 8), rows(8, 8))
    edge_rows(0, rows(48, 8), rows(56, 8))
    gains = node_rows(1, rows(16, 16))
    o_eg[1:2] = four(gains[0:1])
    o_ng[1:2] = four(gains[1:2])
    o_ng[0:1] = four(node_rows(0, rows(32, 16))[0:1])
    last = rows(64, 8)
    o_eg[0:1] = four(jnp.concatenate([last[i : i + 1, 0:128] for i in range(4)], axis=1))


def body(*args):
    (node_latent, edge_latent, node_cotangent, ewi, ewo, nwi, nwo, *gains, edge_slot, edge_receiver, send_list, edge_count) = args
    vmem = pl.BlockSpec(memory_space=pltpu.VMEM)
    far = pl.BlockSpec(memory_space=pl.ANY)
    results = pl.pallas_call(
        kernel,
        out_shape=jax.ShapeDtypeStruct((SUMS_AT + 72, D), F32),
        in_specs=[far] * 13,
        out_specs=far,
        scratch_shapes=flat_scratch()[0],
        compiler_params=pltpu.CompilerParams(
            collective_id=0, has_side_effects=True, vmem_limit_bytes=VMEM_LIMIT
        ),
        cost_estimate=pl.CostEstimate(flops=10**10, bytes_accessed=10**7, transcendentals=10**6),
    )(
        node_latent[0],
        edge_latent[0],
        ewi,
        ewo,
        nwi,
        nwo,
        node_cotangent[0],
        edge_count,
        *gains,
        edge_slot.reshape(8, 128),
        edge_receiver.reshape(8, 128),
        send_list,
    )
    outs = (
        (NODES, D),
        (NODES, D),
        (12, 2, D),
        (2, 4, D),
        (2, 8, D),
        (2, 4, D),
        (2, 4),
        (2, 4),
    )
    results = pl.pallas_call(
        finish_kernel,
        out_shape=tuple(jax.ShapeDtypeStruct(shape, F32) for shape in outs),
        in_specs=[vmem],
        out_specs=tuple([vmem] * 8),
        compiler_params=pltpu.CompilerParams(vmem_limit_bytes=VMEM_LIMIT),
    )(results)
    return (results[0][None], results[1][None], jnp.transpose(results[2], (1, 0, 2))) + tuple(results[3:])


def solution(mesh):
    nodes = P(AXES[1], AXES[0], None)
    graph = P(AXES[0])
    in_specs = (nodes, nodes, nodes) + (P(),) * 6 + (graph, graph, P(AXES[0], None), graph)
    rows = P(None, AXES, None)
    out_specs = (nodes, nodes) + (rows,) * 4 + (P(None, AXES),) * 2
    return jax.shard_map(body, mesh=mesh, in_specs=in_specs, out_specs=out_specs, check_vma=False)
```

```python
import types

import jax
import jax.numpy as jnp
from jax import lax
from jax.experimental import pallas as pl
from jax.experimental.pallas import tpu as pltpu
from jax.sharding import PartitionSpec as P

HOPS = 2
EPSILON = 1e-05
BF = jnp.bfloat16
F32 = jnp.float32
D = 512
NODES = 128
EDGES = 1024
PEER = 32
GROUP = 32
SAMPLES = 4
VMEM_LIMIT = 62 * 1024 * 1024
OFFSETS = tuple(o for o in range(-HOPS, HOPS + 1) if o != 0) + (GROUP // 2,)
HALO = len(OFFSETS) * PEER
RECV_AT = NODES
HALO_AT = 2 * NODES
SUMS_AT = 2 * NODES
FIRST, FORE, BACK = 1024, 1024, 1024
FORE_UNROLL, BACK_UNROLL = 1, 1
MESH = pl.DeviceIdType.MESH
STREAM_TILES = (
    ((16, 384), (16, 384), (32, 128)),
    ((8, 384), (8, 384), (16, 128)),
    ((8, 384), (8, 384), (24, 128)),
)
PART_ORDER = ((1, 2, 0), (2, 0, 1), (0, 1, 2))
AXES = ("graph", "batch")
scope = jax.named_scope


def dot(a, b):
    return jnp.dot(a, b, preferred_element_type=F32)


def dot_tb(a, b):
    return lax.dot_general(a, b, (((1,), (1,)), ((), ())), preferred_element_type=F32)


def dot_ta(a, b):
    return lax.dot_general(a, b, (((0,), (0,)), ((), ())), preferred_element_type=F32)


def place_id(graph, batch):
    return dict(zip(AXES, (graph, batch)))


def wrap(value, size):
    return lax.rem(value + 2 * size, size)


def iota(shape, dim):
    return lax.broadcasted_iota(jnp.int32, shape, dim)


def half_shape(part):
    first, second, _ = PART_ORDER[part]
    shape = [4, 4, 4]
    shape[second] = 2
    del shape[first]
    return tuple(shape)


NL, EWI, EL, EWO, NWI, NWO, COT = 0, (1, 6), 2, (3, 7), (4, 8), (5, 9), 10


def scratch_spec():
    vm = pltpu.VMEM

    def two(shape, dtype):
        return [vm(shape, dtype), vm(shape, dtype)]

    def parts(shape):
        keys = [(stream, part) for stream in range(3) for part in range(3)]
        return {key: vm(shape(key[1]) + STREAM_TILES[key[0]][key[1]], BF) for key in keys}

    return dict(
        nl=vm((NODES, D), BF),
        el=vm((EDGES, D), BF),
        ewi=vm((2, 3 * D, D), BF),
        ewo=vm((2, D, D), BF),
        nwi=vm((2, 2 * D, D), BF),
        nwo=vm((2, D, D), BF),
        cot=vm((NODES, D), BF),
        cnt=pltpu.SMEM((1,), jnp.int32),
        small=[
            vm((2, D), F32),
            vm((2, D), F32),
            vm((8, 128), jnp.int32),
            vm((8, 128), jnp.int32),
            vm((GROUP, PEER), jnp.int32),
        ],
        SR=vm((EDGES, 512), BF),
        SRT=vm((512, EDGES), BF),
        LT=vm((NODES, HALO), BF),
        PS=vm((512, D), BF),
        PRE=vm((EDGES, D), F32),
        EB1=vm((EDGES, D), BF),
        VB1=vm((NODES, D), BF),
        V1=vm((NODES, D), F32),
        NPRE=vm((NODES, D), F32),
        N=two((EDGES, D), BF),
        DA=two((EDGES, D), BF),
        H=two((EDGES, D), BF),
        INV=two((EDGES, 1), F32),
        NN=two((NODES, D), F32),
        NDA=two((NODES, D), F32),
        NH=two((NODES, D), BF),
        NINV=two((NODES, 1), F32),
        AGG=two((NODES, D), BF),
        HS=two((HALO, D), BF),
        HR=two((HALO, D), BF),
        BS=two((HALO, D), BF),
        BR=two((HALO, D), BF),
        G=parts(lambda part: (4, 4, 2, 4)),
        RC=parts(lambda part: (4, 4, 4)),
        RA=parts(lambda part: (6,) + half_shape(part)),
        CA=parts(lambda part: (2,) + half_shape(part)),
        AB=parts(lambda part: (4, 4)),
        RB=parts(lambda part: (3, 4)),
        AD=parts(lambda part: (4,)),
        RD=parts(lambda part: (3,)),
        GZ=vm((EDGES, D), BF),
        GA=vm((EDGES, D), BF),
        GSR=vm((HALO_AT, D), F32),
        GV=vm((NODES, D), F32),
        GACC=vm((8, D), F32),
        WE=vm((3 * D, D), F32),
        WEO=vm((D, D), F32),
        WN=vm((2 * D, D), F32),
        WNO=vm((D, D), F32),
        OUT=vm((SUMS_AT + 72, D), F32),
        store=pltpu.SemaphoreType.DMA((3,)),
        load=pltpu.SemaphoreType.DMA((17,)),
        halo_send=pltpu.SemaphoreType.DMA((2, 2)),
        halo_recv=pltpu.SemaphoreType.DMA((2, 2)),
        rs_send=pltpu.SemaphoreType.DMA((3, 3, 5)),
        rs_recv=pltpu.SemaphoreType.DMA((3, 3, 5)),
    )


def flat_scratch():
    return jax.tree.flatten(scratch_spec())


def kernel(*refs):
    far, out = refs[:13], refs[13]
    r = types.SimpleNamespace(**jax.tree.unflatten(flat_scratch()[1], refs[14:]))
    g = lax.axis_index(AXES[0])
    y = lax.axis_index(AXES[1])
    core = lax.rem(g, 2)
    x = lax.rem(g // 2, 4)
    z = g // 8
    place = (z, x, y)

    def peer(axis, step):
        zz = wrap(z + step, 4) if axis == 0 else z
        xx = wrap(x + step, 4) if axis == 1 else x
        yy = wrap(y + step, 4) if axis == 2 else y
        return place_id((zz * 4 + xx) * 2 + core, yy)

    def graph_peer(offset):
        return place_id(wrap(g + offset, GROUP), y)

    other_core = place_id(g + 1 - 2 * core, y)

    barrier = pltpu.get_barrier_semaphore()
    greeted = 0
    for offset in OFFSETS:
        pl.semaphore_signal(barrier, inc=1, device_id=graph_peer(offset), device_id_type=MESH)
        pl.semaphore_signal(barrier, inc=1, device_id=graph_peer(-offset), device_id_type=MESH)
        greeted += 2
    for axis in range(3):
        for step in (1, 2, 3):
            pl.semaphore_signal(barrier, inc=1, device_id=peer(axis, step), device_id_type=MESH)
            greeted += 1
    pl.semaphore_signal(barrier, inc=1, device_id=other_core, device_id_type=MESH)
    greeted += 1

    nl, el, ewi, ewo, nwi, nwo, cot, cnt, *small = far
    pairs = [(nl, r.nl), (ewi, r.ewi, 0), (el, r.el), (ewo, r.ewo, 0), (nwi, r.nwi, 0), (nwo, r.nwo, 0)]
    pairs += [(ewi, r.ewi, 1), (ewo, r.ewo, 1), (nwi, r.nwi, 1), (nwo, r.nwo, 1), (cot, r.cot), (cnt, r.cnt)]
    eg, ng, slot, rcv, slist = r.small
    pairs += list(zip(small, r.small))

    def load(number):
        src, dst, *layer = pairs[number]
        if layer:
            src, dst = src.at[layer[0]], dst.at[layer[0]]
        return pltpu.make_async_copy(src, dst, r.load.at[number])

    for number in (16, 0, 14, 15, 11) + tuple(range(1, 11)) + (12, 13):
        load(number).start()

    load(16).wait()
    listed = jnp.concatenate(
        [slist[pl.ds(wrap(g - offset, GROUP), 1), :] for offset in OFFSETS], axis=1
    ).astype(F32)
    node_ids = iota((NODES, HALO), 0).astype(F32)
    r.LT[...] = jnp.where(node_ids == listed, 1.0, 0.0).astype(BF)

    def remote(src, dst, send_sem, recv_sem, device):
        return pltpu.make_async_remote_copy(
            src_ref=src,
            dst_ref=dst,
            send_sem=send_sem,
            recv_sem=recv_sem,
            device_id=device,
            device_id_type=MESH,
        )

    def halo_copies(layer, way):
        src, dst = ((r.HS, r.HR), (r.BS, r.BR))[way]
        src, dst = src[layer], dst[layer]
        copies = []
        for b in reversed(range(len(OFFSETS))):
            offset = OFFSETS[b]
            rows = pl.ds(b * PEER, PEER)
            copies.append(
                remote(
                    src.at[rows],
                    dst.at[rows],
                    r.halo_send.at[layer, way],
                    r.halo_recv.at[layer, way],
                    graph_peer(-offset if way == 0 else offset),
                )
            )
        return copies, remote(src, dst, r.halo_send.at[layer, way], r.halo_recv.at[layer, way], other_core)

    def vb(layer):
        return r.nl if layer == 0 else r.VB1

    def eb(layer):
        return r.el if layer == 0 else r.EB1

    def one_hots():
        for number in (11, 14, 15):
            load(number).wait()
        s = slot[...]
        within = s - NODES
        source = within // PEER
        distance = wrap(source - g, GROUP)
        block = jnp.zeros_like(s)
        for b, offset in enumerate(OFFSETS):
            block = jnp.where(distance == offset % GROUP, b, block)
        position = jnp.where(s < NODES, s, HALO_AT + block * PEER + (within - source * PEER))
        edge = iota((8, 128), 0) * 128 + iota((8, 128), 1)
        receiver = jnp.where(edge < r.cnt[0], rcv[...] + RECV_AT, -1)
        position = position.astype(F32)
        receiver = receiver.astype(F32)
        row_ids = iota((512, 128), 0).astype(F32)
        lane_ids = iota((128, 512), 1).astype(F32)
        for i in range(8):
            prow = position[i : i + 1, :]
            rrow = receiver[i : i + 1, :]
            at = slice(i * 128, (i + 1) * 128)
            for j in range(4):
                rows = slice(j * 128, (j + 1) * 128)
                row = rrow if j == 1 else prow
                r.SRT[rows, at] = jnp.where(row_ids[rows] == row, 1.0, 0.0).astype(BF)
            pcol = jnp.broadcast_to(prow, (128, 128)).T
            rcol = jnp.broadcast_to(rrow, (128, 128)).T
            for j in range(4):
                col = rcol if j == 1 else pcol
                lanes = slice(j * 128, (j + 1) * 128)
                r.SR[at, lanes] = jnp.where(lane_ids[:, lanes] == col, 1.0, 0.0).astype(BF)

    def norm(projected):
        centre = projected - jnp.mean(projected, axis=-1, keepdims=True)
        inv_std = lax.rsqrt(jnp.mean(centre * centre, axis=-1, keepdims=True) + EPSILON)
        return centre * inv_std, inv_std

    def swish(pre_act):
        sigma = 0.5 * jnp.tanh(0.5 * pre_act) + 0.5
        hidden = pre_act * sigma
        return hidden, sigma + hidden * (1.0 - sigma)

    def tile_at(t, rows):
        return pl.ds(pl.multiple_of(t * rows, rows), rows)

    def forward(layer):
        w = r.ewi.at[layer]
        wo = r.ewo.at[layer]
        nw = r.nwi.at[layer]
        nwo = r.nwo.at[layer]
        ps = r.PS
        with scope("f_send"):
            if layer == 0:
                load(NL).wait()
            r.HS[layer][...] = dot_ta(r.LT[...], vb(layer)[...]).astype(BF)
            copies, all_rows = halo_copies(layer, 0)
            if layer == 0:
                pl.semaphore_wait(barrier, greeted)
            for copy in copies:
                copy.start()
        with scope("f_first"):
            if layer == 0:
                one_hots()
            node = vb(layer)[...]
            load(EWI[layer]).wait()
            ps[0:NODES] = dot(node, w[D : 2 * D]).astype(BF)
            ps[RECV_AT:HALO_AT] = dot(node, w[2 * D :]).astype(BF)
            if layer == 0:
                ps[HALO_AT + HALO :] = jnp.zeros((512 - HALO_AT - HALO, D), BF)
                load(EL).wait()

            def first(t, carry):
                at = tile_at(t, FIRST)
                r.PRE[at] = dot(eb(layer)[at], w[0:D]) + dot(r.SR[at, 0:HALO_AT], ps[0:HALO_AT])
                return carry

            lax.fori_loop(0, EDGES // FIRST, first, 0)
            load(NWI[layer]).wait()
            r.NPRE[...] = dot(node, nw[0:D])
        with scope("f_halo_wait"):
            load(EWO[layer]).wait()
            load(NWO[layer]).wait()
            all_rows.wait()
        with scope("f_edges"):
            if layer == 0:
                load(12).wait()
                load(13).wait()
            gain = eg[layer : layer + 1, :]
            ps[HALO_AT : HALO_AT + HALO] = dot(r.HR[layer][...], w[D : 2 * D]).astype(BF)

            def edges(t, carry):
                at = tile_at(t, FORE)
                pre_act = r.PRE[at] + dot(r.SR[at, HALO_AT:], ps[HALO_AT:])
                hidden, slope = swish(pre_act)
                hidden = hidden.astype(BF)
                r.H[layer][at] = hidden
                r.DA[layer][at] = slope.astype(BF)
                normed, inv_std = norm(dot(hidden, wo[...]))
                r.INV[layer][at] = inv_std
                r.N[layer][at] = normed.astype(BF)
                if layer == 0:
                    r.EB1[at] = (r.el[at].astype(F32) + normed * gain).astype(BF)
                return carry

            lax.fori_loop(0, EDGES // FORE, edges, 0, unroll=FORE_UNROLL)
        with scope("f_node"):
            agg = (dot(r.SRT[RECV_AT:HALO_AT], r.N[layer][...]) * gain).astype(BF)
            r.AGG[layer][...] = agg
            pre_act = r.NPRE[...] + dot(agg, nw[D:])
            hidden, slope = swish(pre_act)
            hidden = hidden.astype(BF)
            r.NH[layer][...] = hidden
            r.NDA[layer][...] = slope
            normed, inv_std = norm(dot(hidden, nwo[...]))
            r.NN[layer][...] = normed
            r.NINV[layer][...] = inv_std
            update = normed * ng[layer : layer + 1, :]
            if layer == 0:
                state = r.nl[...].astype(F32) + update
                r.V1[...] = state
                r.VB1[...] = state.astype(BF)
            else:
                r.OUT[0:NODES] = r.V1[...] + update

    def norm_back(grad, normed, inv_std):
        return inv_std * (
            grad
            - jnp.mean(grad, axis=-1, keepdims=True)
            - normed * jnp.mean(grad * normed, axis=-1, keepdims=True)
        )

    def fold_rows(a):
        return jnp.sum(a.reshape(a.shape[0] // 8, 8, a.shape[1]), axis=0)

    def backward_nodes(layer):
        nw = r.nwi.at[layer]
        node = vb(layer)[...]
        with scope("b_node"):
            grad = r.GV[...]
            normed = r.NN[layer][...]
            gain_sum = jnp.sum(grad * normed, axis=0, keepdims=True)
            gz = norm_back(grad * ng[layer : layer + 1, :], normed, r.NINV[layer][...]).astype(BF)
            ga = (dot_tb(gz, r.nwo[layer]) * r.NDA[layer][...]).astype(BF)
            grad_agg = dot_tb(ga, nw[D:]).astype(BF)
            r.GACC[...] = jnp.zeros((8, D), F32)

        def weights():
            with scope("b_dwn"):
                r.WN[0:D] = dot_ta(node, ga)
                r.WN[D:] = dot_ta(r.AGG[layer][...], ga)
                r.WNO[...] = dot_ta(r.NH[layer][...], gz)
                r.GV[...] = r.GV[...] + dot_tb(ga, nw[0:D])

        return grad_agg, gain_sum, weights

    def backward_edges(layer, grad_agg):
        wo = r.ewo.at[layer]
        gain = eg[layer : layer + 1, :]

        def edges(t, carry):
            at = tile_at(t, BACK)
            gm = dot(r.SR[at, RECV_AT:HALO_AT], grad_agg)
            if layer == 0:
                gm = gm + r.PRE[at]
            en = r.N[layer][at].astype(F32)
            r.GACC[...] += fold_rows(gm * en)
            ez = norm_back(gm * gain, en, r.INV[layer][at]).astype(BF)
            r.GZ[at] = ez
            ea = (dot_tb(ez, wo[...]) * r.DA[layer][at].astype(F32)).astype(BF)
            r.GA[at] = ea
            return carry

        with scope("b_edges"):
            lax.fori_loop(0, EDGES // BACK, edges, 0, unroll=BACK_UNROLL)

    def return_halo(layer):
        with scope("b_gsr"):
            sums = dot(r.SRT[...], r.GA[...])
            r.GSR[...] = sums[0:HALO_AT]
            r.BS[layer][...] = sums[HALO_AT : HALO_AT + HALO].astype(BF)
            copies, all_rows = halo_copies(layer, 1)
            for copy in copies:
                copy.start()
        return all_rows

    def edge_weights(layer):
        node = vb(layer)[...]
        with scope("b_dwe"):
            r.WE[0:D] = dot_ta(eb(layer)[...], r.GA[...])
            r.WEO[...] = dot_ta(r.H[layer][...], r.GZ[...])
            to_sender = r.GSR[0:NODES].astype(BF)
            to_receiver = r.GSR[RECV_AT:HALO_AT].astype(BF)
            r.WE[D : 2 * D] = dot_ta(node, to_sender) + dot_ta(r.HR[layer][...], r.BS[layer][...])
            r.WE[2 * D :] = dot_ta(node, to_receiver)
        return jnp.sum(r.GACC[...], axis=0, keepdims=True)

    def edge_inputs(layer):
        with scope("b_inputs"):
            to_receiver = r.GSR[RECV_AT:HALO_AT].astype(BF)
            r.GV[...] = r.GV[...] + dot_tb(to_receiver, r.ewi[layer, 2 * D :])
            if layer == 1:
                r.PRE[...] = dot_tb(r.GA[...], r.ewi[layer, 0:D])

    def take_halo(layer, copies):
        w = r.ewi.at[layer]
        with scope("b_halo_wait"):
            copies.wait()
        with scope("b_tail"):
            to_sender = (r.GSR[0:NODES] + dot(r.LT[...], r.BR[layer][...])).astype(BF)
            total = r.GV[...] + dot_tb(to_sender, w[D : 2 * D])
            r.GV[...] = total
        return total

    low = iota((8, D), 0) < 4

    def each_pair(make):
        def slab(zz, carry):
            for xx in range(4):
                for cc in range(2):
                    for yy in range(2):
                        make((zz, xx, cc), 2 * yy, (zz, (xx * 2 + cc) * 2 + yy))
            return carry

        lax.fori_loop(0, 4, slab, 0)

    def pair_rows(ref, k, start, size):
        zz, inner = k
        return ref[pl.ds(pl.multiple_of(zz * 16 * size, 8) + inner * size + start, 8), :]

    def edge_slots(k):
        e0, e1, e2 = (pair_rows(r.WE, k, 8 * i, 24) for i in range(3))
        out = pltpu.roll(pair_rows(r.WEO, k, 0, 8), 4, 0)
        return (e0, jnp.where(low, e1, out)), (e2, jnp.where(low, out, e1))

    def assemble_edges(layer, gain_sum):
        def pair(where, yy, k):
            for odd, (g0, g1) in enumerate(edge_slots(k)):
                at = where + (yy + odd,)
                if layer == 1:
                    both = jnp.concatenate([g0, g1], axis=0).astype(BF)
                    r.G[0, 0][at] = both[:, 0:384]
                    r.G[0, 2][at + (slice(0, 16),)] = both[:, 384:]
                else:
                    r.G[2, 0][at] = g0[:, 0:384].astype(BF)
                    r.G[2, 1][at] = g1[:, 0:384].astype(BF)
                    r.G[2, 2][at] = jnp.concatenate([g0[:, 384:], g1[:, 384:], gains], axis=0).astype(BF)

        if layer == 0:
            lanes = [gain_sum[:, 128 * i : 128 * (i + 1)] for i in range(4)]
            gains = jnp.zeros((8, 128), F32)
            for i in range(4):
                gains = jnp.where(iota((8, 128), 0) == i, lanes[i], gains)
        with scope("asm_edges"):
            each_pair(pair)

    def assemble_nodes(layer, *gain_sums):
        row = iota((8, D), 0) % 4
        gains = jnp.zeros((8, D), F32)
        for i, gain_sum in enumerate(gain_sums):
            gains = jnp.where(row == i, gain_sum, gains)
        def pair(where, yy, k):
            n0, n1 = (pair_rows(r.WN, k, 8 * i, 16) for i in range(2))
            last = pair_rows(r.WNO, k, 0, 8)
            slots = ((n0, jnp.where(low, last, gains)), (n1, jnp.where(low, gains, last)))
            for odd, (g2, g3) in enumerate(slots):
                at = where + (yy + odd,)
                if layer == 1:
                    both = jnp.concatenate([g2, g3], axis=0).astype(BF)
                    r.G[0, 1][at] = both[:, 0:384]
                    r.G[0, 2][at + (slice(16, 32),)] = both[:, 384:]
                else:
                    r.G[1, 0][at] = g2[:, 0:384].astype(BF)
                    r.G[1, 1][at] = g3[:, 0:384].astype(BF)
                    r.G[1, 2][at] = jnp.concatenate([g2[:, 384:], g3[:, 384:]], axis=0).astype(BF)

        with scope("asm_nodes"):
            each_pair(pair)

    def rs_copy(key, number, src, dst, device):
        return remote(src, dst, r.rs_send.at[key[0], key[1], number], r.rs_recv.at[key[0], key[1], number], device)

    def settle(key, number, ref):
        rs_copy(key, number, ref, ref, other_core).wait()

    def cores(key):
        return rs_copy(key, 0, r.G[key].at[:, :, 1 - core], r.RC[key], other_core)

    def axes(key):
        first, second, third = PART_ORDER[key[1]]
        return first, second, third, second - (1 if first < second else 0)

    def cut(key, first_at, half):
        first, second, _, _ = axes(key)
        index = [slice(None)] * 3
        index[first] = first_at
        index[second] = pl.ds(2 * half, 2)
        return tuple(index)

    def ring(key, slot):
        axis = axes(key)[0]
        me = place[axis]
        way, kind = slot // 3, slot % 3
        sign = 1 - 2 * way
        if kind == 0:
            src = r.RC[key].at[cut(key, wrap(me + 2, 4), 1 - way)]
        elif kind == 1:
            src = r.RC[key].at[cut(key, wrap(me + sign, 4), way)]
        else:
            src = r.CA[key].at[way]
        return rs_copy(key, 1 if kind == 0 else 2, src, r.RA[key].at[slot], peer(axis, sign))

    def second_copies(key):
        _, axis, _, at = axes(key)
        copies = []
        for step in (2, 1, 3):
            src = r.AB[key].at[(slice(None),) * at + (wrap(place[axis] + step, 4),)]
            copies.append(rs_copy(key, 3, src, r.RB[key].at[step - 1], peer(axis, step)))
        return copies

    def third_copies(key):
        axis = axes(key)[2]
        copies = []
        for step in (2, 1, 3):
            src = r.AD[key].at[wrap(place[axis] + step, 4)]
            copies.append(rs_copy(key, 4, src, r.RD[key].at[step - 1], peer(axis, step)))
        return copies

    def rs_cores(key):
        cores(key).start()

    def rs_ring(key):
        with scope("rs_ring"):
            cores(key).wait()
            mine, both = r.G[key], r.RC[key]

            def add(i, carry):
                both[i] = both[i] + mine[i, :, core]
                return carry

            lax.fori_loop(0, 4, add, 0)
            for slot in (0, 3, 1, 4):
                ring(key, slot).start()

    def rs_sums(key):
        with scope("rs_sums"):
            me = place[axes(key)[0]]
            got = r.RA[key]
            settle(key, 1, got.at[0:2])
            for way, sign in ((0, 1), (1, -1)):
                own = r.RC[key][cut(key, wrap(me + sign, 4), 1 - way)]
                r.CA[key][way] = own + got[3 * way]
                ring(key, 3 * way + 2).start()

    def rs_second(key):
        with scope("rs_second"):
            first, axis, _, at = axes(key)
            got = r.RA[key]
            settle(key, 2, got.at[0:4])
            for half in range(2):
                near, summed = (1, 5) if half == 0 else (4, 2)
                total = r.RC[key][cut(key, place[first], half)].astype(F32)
                total = total + got[near].astype(F32) + got[summed].astype(F32)
                index = (slice(None),) * at + (slice(2 * half, 2 * half + 2),)
                r.AB[key][index] = total.astype(BF)
            for copy in second_copies(key):
                copy.start()

    def rs_third(key):
        with scope("rs_third"):
            _, axis, _, at = axes(key)
            settle(key, 3, r.RB[key])
            total = r.AB[key][(slice(None),) * at + (place[axis],)].astype(F32)
            for i in range(3):
                total = total + r.RB[key][i].astype(F32)
            r.AD[key][...] = total.astype(BF)
            for copy in third_copies(key):
                copy.start()

    def rs_finish(key):
        with scope("rs_finish"):
            settle(key, 4, r.RD[key])
            total = r.AD[key][place[axes(key)[2]]].astype(F32)
            for i in range(3):
                total = total + r.RD[key][i].astype(F32)
            stream, part = key
            start = SUMS_AT + (0, 32, 48)[stream]
            rows = 16 if stream == 0 else 8
            if part < 2:
                r.OUT[start + rows * part : start + rows * part + rows, 0:384] = total
            else:
                r.OUT[start : start + 2 * rows, 384:] = total[0 : 2 * rows]
            if key == (2, 2):
                r.OUT[SUMS_AT + 64 :, 0:128] = total[16:24]

    def store(number):
        rows = pl.ds((0, NODES, SUMS_AT)[number], (NODES, NODES, 72)[number])
        return pltpu.make_async_copy(r.OUT.at[rows], out.at[rows], r.store.at[number])

    def each(call, stream, *parts):
        for part in parts or range(3):
            call((stream, part))

    forward(0)
    forward(1)
    store(0).start()
    load(COT).wait()
    r.GV[...] = r.cot[...].astype(F32)

    grad_agg, node_gain, node_weights = backward_nodes(1)
    backward_edges(1, grad_agg)
    copies = return_halo(1)
    edge_gain = edge_weights(1)
    assemble_edges(1, None)
    each(rs_cores, 0, 0)
    edge_inputs(1)
    node_weights()
    assemble_nodes(1, edge_gain, node_gain)
    each(rs_cores, 0, 1, 2)
    take_halo(1, copies)
    each(rs_ring, 0, 0)

    grad_agg, node_gain, node_weights = backward_nodes(0)
    node_weights()
    assemble_nodes(0, node_gain)
    each(rs_cores, 1)
    each(rs_ring, 0, 1, 2)
    backward_edges(0, grad_agg)
    copies = return_halo(0)
    each(rs_ring, 1)
    each(rs_sums, 0, 0)
    edge_gain = edge_weights(0)
    assemble_edges(0, edge_gain)
    each(rs_cores, 2)
    each(rs_sums, 0, 1, 2)
    edge_inputs(0)
    each(rs_ring, 2)
    each(rs_sums, 1)
    each(rs_second, 0)
    each(rs_sums, 2)
    each(rs_second, 1)
    r.OUT[NODES : 2 * NODES] = take_halo(0, copies)
    store(1).start()
    each(rs_third, 0)
    each(rs_second, 2)
    each(rs_third, 1)
    each(rs_third, 2)
    for stream in range(3):
        each(rs_finish, stream)
    with scope("z_store"):
        store(2).start()
        for number in range(3):
            store(number).wait()


def finish_kernel(sums, o_node, o_grad, o_ei, o_eo, o_ni, o_no, o_eg, o_ng):
    y = lax.axis_index(AXES[1])
    column = (lax.axis_index(AXES[0]) * SAMPLES + y) * 4
    is_even = lax.rem(y, 2) == 0
    o_node[...] = sums[0:NODES]
    o_grad[...] = sums[NODES : 2 * NODES]

    def edge_rows(layer, g0, g1):
        even = jnp.concatenate([g0, g1[0:4]], axis=0)
        odd = jnp.concatenate([g1[4:8], g0], axis=0)
        o_ei[:, layer] = jnp.where(is_even, even, odd)
        o_eo[layer] = jnp.where(is_even, g1[4:8], g1[0:4])

    def node_rows(layer, total):
        o_ni[layer] = total[0:8]
        last = total[8:16]
        o_no[layer] = jnp.where(is_even, last[0:4], last[4:8])
        return jnp.where(is_even, last[4:8], last[0:4])

    def four(row):
        lane = iota((1, D), 1)
        at = iota((1, 4), 1)
        picked = jnp.zeros((1, 4), F32)
        for i in range(4):
            value = jnp.sum(jnp.where(lane == column + i, row, 0.0), axis=1, keepdims=True)
            picked = jnp.where(at == i, value, picked)
        return picked

    def rows(start, size):
        return sums[SUMS_AT + start : SUMS_AT + start + size]

    edge_rows(1, rows(0, 8), rows(8, 8))
    edge_rows(0, rows(48, 8), rows(56, 8))
    gains = node_rows(1, rows(16, 16))
    o_eg[1:2] = four(gains[0:1])
    o_ng[1:2] = four(gains[1:2])
    o_ng[0:1] = four(node_rows(0, rows(32, 16))[0:1])
    last = rows(64, 8)
    o_eg[0:1] = four(jnp.concatenate([last[i : i + 1, 0:128] for i in range(4)], axis=1))


def body(*args):
    (node_latent, edge_latent, node_cotangent, ewi, ewo, nwi, nwo, *gains, edge_slot, edge_receiver, send_list, edge_count) = args
    vmem = pl.BlockSpec(memory_space=pltpu.VMEM)
    far = pl.BlockSpec(memory_space=pl.ANY)
    results = pl.pallas_call(
        kernel,
        out_shape=jax.ShapeDtypeStruct((SUMS_AT + 72, D), F32),
        in_specs=[far] * 13,
        out_specs=far,
        scratch_shapes=flat_scratch()[0],
        compiler_params=pltpu.CompilerParams(
            collective_id=0, has_side_effects=True, vmem_limit_bytes=VMEM_LIMIT
        ),
        cost_estimate=pl.CostEstimate(flops=10**10, bytes_accessed=10**7, transcendentals=10**6),
    )(
        node_latent[0],
        edge_latent[0],
        ewi,
        ewo,
        nwi,
        nwo,
        node_cotangent[0],
        edge_count,
        *gains,
        edge_slot.reshape(8, 128),
        edge_receiver.reshape(8, 128),
        send_list,
    )
    outs = (
        (NODES, D),
        (NODES, D),
        (12, 2, D),
        (2, 4, D),
        (2, 8, D),
        (2, 4, D),
        (2, 4),
        (2, 4),
    )
    results = pl.pallas_call(
        finish_kernel,
        out_shape=tuple(jax.ShapeDtypeStruct(shape, F32) for shape in outs),
        in_specs=[vmem],
        out_specs=tuple([vmem] * 8),
        compiler_params=pltpu.CompilerParams(vmem_limit_bytes=VMEM_LIMIT),
    )(results)
    return (results[0][None], results[1][None], jnp.transpose(results[2], (1, 0, 2))) + tuple(results[3:])


def solution(mesh):
    nodes = P(AXES[1], AXES[0], None)
    graph = P(AXES[0])
    in_specs = (nodes, nodes, nodes) + (P(),) * 6 + (graph, graph, P(AXES[0], None), graph)
    rows = P(None, AXES, None)
    out_specs = (nodes, nodes) + (rows,) * 4 + (P(None, AXES),) * 2
    return jax.shard_map(body, mesh=mesh, in_specs=in_specs, out_specs=out_specs, check_vma=False)
```

```python
import types

import jax
import jax.numpy as jnp
from jax import lax
from jax.experimental import pallas as pl
from jax.experimental.pallas import tpu as pltpu
from jax.sharding import PartitionSpec as P

HOPS = 2
EPSILON = 1e-05
BF = jnp.bfloat16
F32 = jnp.float32
D = 512
NODES = 128
EDGES = 1024
PEER = 32
GROUP = 32
SAMPLES = 4
VMEM_LIMIT = 62 * 1024 * 1024
OFFSETS = tuple(o for o in range(-HOPS, HOPS + 1) if o != 0) + (GROUP // 2,)
HALO = len(OFFSETS) * PEER
RECV_AT = NODES
HALO_AT = 2 * NODES
SUMS_AT = 2 * NODES
FIRST, FORE, BACK = 1024, 1024, 1024
FORE_UNROLL, BACK_UNROLL = 1, 1
MESH = pl.DeviceIdType.MESH
STREAM_TILES = (
    ((16, 384), (16, 384), (32, 128)),
    ((8, 384), (8, 384), (16, 128)),
    ((8, 384), (8, 384), (24, 128)),
)
PART_ORDER = ((1, 2, 0), (2, 0, 1), (0, 1, 2))
AXES = ("graph", "batch")
scope = jax.named_scope


def dot(a, b):
    return jnp.dot(a, b, preferred_element_type=F32)


def dot_tb(a, b):
    return lax.dot_general(a, b, (((1,), (1,)), ((), ())), preferred_element_type=F32)


def dot_ta(a, b):
    return lax.dot_general(a, b, (((0,), (0,)), ((), ())), preferred_element_type=F32)


def place_id(graph, batch):
    return dict(zip(AXES, (graph, batch)))


def wrap(value, size):
    return lax.rem(value + 2 * size, size)


def iota(shape, dim):
    return lax.broadcasted_iota(jnp.int32, shape, dim)


def half_shape(part):
    first, second, _ = PART_ORDER[part]
    shape = [4, 4, 4]
    shape[second] = 2
    del shape[first]
    return tuple(shape)


NL, EWI, EL, EWO, NWI, NWO, COT = 0, (1, 6), 2, (3, 7), (4, 8), (5, 9), 10


def scratch_spec():
    vm = pltpu.VMEM

    def two(shape, dtype):
        return [vm(shape, dtype), vm(shape, dtype)]

    def parts(shape):
        keys = [(stream, part) for stream in range(3) for part in range(3)]
        return {key: vm(shape(key[1]) + STREAM_TILES[key[0]][key[1]], BF) for key in keys}

    return dict(
        nl=vm((NODES, D), BF),
        el=vm((EDGES, D), BF),
        ewi=vm((2, 3 * D, D), BF),
        ewo=vm((2, D, D), BF),
        nwi=vm((2, 2 * D, D), BF),
        nwo=vm((2, D, D), BF),
        cot=vm((NODES, D), BF),
        cnt=pltpu.SMEM((1,), jnp.int32),
        small=[
            vm((2, D), F32),
            vm((2, D), F32),
            vm((8, 128), jnp.int32),
            vm((8, 128), jnp.int32),
            vm((GROUP, PEER), jnp.int32),
        ],
        SR=vm((EDGES, 512), BF),
        SRT=vm((512, EDGES), BF),
        LT=vm((NODES, HALO), BF),
        PS=vm((512, D), BF),
        PRE=vm((EDGES, D), F32),
        EB1=vm((EDGES, D), BF),
        VB1=vm((NODES, D), BF),
        V1=vm((NODES, D), F32),
        NPRE=vm((NODES, D), F32),
        N=two((EDGES, D), BF),
        DA=two((EDGES, D), BF),
        H=two((EDGES, D), BF),
        INV=two((EDGES, 1), F32),
        NN=two((NODES, D), F32),
        NDA=two((NODES, D), F32),
        NH=two((NODES, D), BF),
        NINV=two((NODES, 1), F32),
        AGG=two((NODES, D), BF),
        HS=two((HALO, D), BF),
        HR=two((HALO, D), BF),
        BS=two((HALO, D), BF),
        BR=two((HALO, D), BF),
        G=parts(lambda part: (4, 4, 2, 4)),
        RC=parts(lambda part: (4, 4, 4)),
        RA=parts(lambda part: (6,) + half_shape(part)),
        CA=parts(lambda part: (2,) + half_shape(part)),
        AB=parts(lambda part: (4, 4)),
        RB=parts(lambda part: (3, 4)),
        AD=parts(lambda part: (4,)),
        RD=parts(lambda part: (3,)),
        GZ=vm((EDGES, D), BF),
        GA=vm((EDGES, D), BF),
        GSR=vm((HALO_AT, D), F32),
        GV=vm((NODES, D), F32),
        GACC=vm((8, D), F32),
        WE=vm((3 * D, D), F32),
        WEO=vm((D, D), F32),
        WN=vm((2 * D, D), F32),
        WNO=vm((D, D), F32),
        OUT=vm((SUMS_AT + 72, D), F32),
        store=pltpu.SemaphoreType.DMA((3,)),
        load=pltpu.SemaphoreType.DMA((17,)),
        halo_send=pltpu.SemaphoreType.DMA((2, 2)),
        halo_recv=pltpu.SemaphoreType.DMA((2, 2)),
        rs_send=pltpu.SemaphoreType.DMA((3, 3, 5)),
        rs_recv=pltpu.SemaphoreType.DMA((3, 3, 5)),
    )


def flat_scratch():
    return jax.tree.flatten(scratch_spec())


def kernel(*refs):
    far, out = refs[:13], refs[13]
    r = types.SimpleNamespace(**jax.tree.unflatten(flat_scratch()[1], refs[14:]))
    g = lax.axis_index(AXES[0])
    y = lax.axis_index(AXES[1])
    core = lax.rem(g, 2)
    x = lax.rem(g // 2, 4)
    z = g // 8
    place = (z, x, y)

    def peer(axis, step):
        zz = wrap(z + step, 4) if axis == 0 else z
        xx = wrap(x + step, 4) if axis == 1 else x
        yy = wrap(y + step, 4) if axis == 2 else y
        return place_id((zz * 4 + xx) * 2 + core, yy)

    def graph_peer(offset):
        return place_id(wrap(g + offset, GROUP), y)

    other_core = place_id(g + 1 - 2 * core, y)

    nl, el, ewi, ewo, nwi, nwo, cot, cnt, *small = far
    pairs = [(nl, r.nl), (ewi, r.ewi, 0), (el, r.el), (ewo, r.ewo, 0), (nwi, r.nwi, 0), (nwo, r.nwo, 0)]
    pairs += [(ewi, r.ewi, 1), (ewo, r.ewo, 1), (nwi, r.nwi, 1), (nwo, r.nwo, 1), (cot, r.cot), (cnt, r.cnt)]
    eg, ng, slot, rcv, slist = r.small
    pairs += list(zip(small, r.small))

    def load(number):
        src, dst, *layer = pairs[number]
        if layer:
            src, dst = src.at[layer[0]], dst.at[layer[0]]
        return pltpu.make_async_copy(src, dst, r.load.at[number])

    for number in (16, 0):
        load(number).start()

    barrier = pltpu.get_barrier_semaphore()
    greeted = 0
    for offset in OFFSETS:
        pl.semaphore_signal(barrier, inc=1, device_id=graph_peer(offset), device_id_type=MESH)
        pl.semaphore_signal(barrier, inc=1, device_id=graph_peer(-offset), device_id_type=MESH)
        greeted += 2
    for axis in range(3):
        for step in (1, 2, 3):
            pl.semaphore_signal(barrier, inc=1, device_id=peer(axis, step), device_id_type=MESH)
            greeted += 1
    pl.semaphore_signal(barrier, inc=1, device_id=other_core, device_id_type=MESH)
    greeted += 1

    for number in (14, 15, 11) + tuple(range(1, 11)) + (12, 13):
        load(number).start()

    load(16).wait()
    listed = jnp.concatenate(
        [slist[pl.ds(wrap(g - offset, GROUP), 1), :] for offset in OFFSETS], axis=1
    ).astype(F32)
    node_ids = iota((NODES, HALO), 0).astype(F32)
    r.LT[...] = jnp.where(node_ids == listed, 1.0, 0.0).astype(BF)

    def remote(src, dst, send_sem, recv_sem, device):
        return pltpu.make_async_remote_copy(
            src_ref=src,
            dst_ref=dst,
            send_sem=send_sem,
            recv_sem=recv_sem,
            device_id=device,
            device_id_type=MESH,
        )

    def halo_copies(layer, way):
        src, dst = ((r.HS, r.HR), (r.BS, r.BR))[way]
        src, dst = src[layer], dst[layer]
        copies = []
        for b in reversed(range(len(OFFSETS))):
            offset = OFFSETS[b]
            rows = pl.ds(b * PEER, PEER)
            copies.append(
                remote(
                    src.at[rows],
                    dst.at[rows],
                    r.halo_send.at[layer, way],
                    r.halo_recv.at[layer, way],
                    graph_peer(-offset if way == 0 else offset),
                )
            )
        return copies, remote(src, dst, r.halo_send.at[layer, way], r.halo_recv.at[layer, way], other_core)

    def vb(layer):
        return r.nl if layer == 0 else r.VB1

    def eb(layer):
        return r.el if layer == 0 else r.EB1

    def one_hots():
        for number in (11, 14, 15):
            load(number).wait()
        s = slot[...]
        within = s - NODES
        source = within // PEER
        distance = wrap(source - g, GROUP)
        block = jnp.zeros_like(s)
        for b, offset in enumerate(OFFSETS):
            block = jnp.where(distance == offset % GROUP, b, block)
        position = jnp.where(s < NODES, s, HALO_AT + block * PEER + (within - source * PEER))
        edge = iota((8, 128), 0) * 128 + iota((8, 128), 1)
        receiver = jnp.where(edge < r.cnt[0], rcv[...] + RECV_AT, -1)
        position = position.astype(F32)
        receiver = receiver.astype(F32)
        row_ids = iota((512, 128), 0).astype(F32)
        lane_ids = iota((128, 512), 1).astype(F32)
        for i in range(8):
            prow = position[i : i + 1, :]
            rrow = receiver[i : i + 1, :]
            at = slice(i * 128, (i + 1) * 128)
            for j in range(4):
                rows = slice(j * 128, (j + 1) * 128)
                row = rrow if j == 1 else prow
                r.SRT[rows, at] = jnp.where(row_ids[rows] == row, 1.0, 0.0).astype(BF)
            pcol = jnp.broadcast_to(prow, (128, 128)).T
            rcol = jnp.broadcast_to(rrow, (128, 128)).T
            for j in range(4):
                col = rcol if j == 1 else pcol
                lanes = slice(j * 128, (j + 1) * 128)
                r.SR[at, lanes] = jnp.where(lane_ids[:, lanes] == col, 1.0, 0.0).astype(BF)

    def norm(projected):
        centre = projected - jnp.mean(projected, axis=-1, keepdims=True)
        inv_std = lax.rsqrt(jnp.mean(centre * centre, axis=-1, keepdims=True) + EPSILON)
        return centre * inv_std, inv_std

    def swish(pre_act):
        sigma = 0.5 * jnp.tanh(0.5 * pre_act) + 0.5
        hidden = pre_act * sigma
        return hidden, sigma + hidden * (1.0 - sigma)

    def tile_at(t, rows):
        return pl.ds(pl.multiple_of(t * rows, rows), rows)

    def forward(layer):
        w = r.ewi.at[layer]
        wo = r.ewo.at[layer]
        nw = r.nwi.at[layer]
        nwo = r.nwo.at[layer]
        ps = r.PS
        with scope("f_send"):
            if layer == 0:
                load(NL).wait()
            r.HS[layer][...] = dot_ta(r.LT[...], vb(layer)[...]).astype(BF)
            copies, all_rows = halo_copies(layer, 0)
            if layer == 0:
                pl.semaphore_wait(barrier, greeted)
            for copy in copies:
                copy.start()
        with scope("f_first"):
            if layer == 0:
                one_hots()
            node = vb(layer)[...]
            load(EWI[layer]).wait()
            ps[0:NODES] = dot(node, w[D : 2 * D]).astype(BF)
            ps[RECV_AT:HALO_AT] = dot(node, w[2 * D :]).astype(BF)
            if layer == 0:
                ps[HALO_AT + HALO :] = jnp.zeros((512 - HALO_AT - HALO, D), BF)
                load(EL).wait()

            def first(t, carry):
                at = tile_at(t, FIRST)
                r.PRE[at] = dot(eb(layer)[at], w[0:D]) + dot(r.SR[at, 0:HALO_AT], ps[0:HALO_AT])
                return carry

            lax.fori_loop(0, EDGES // FIRST, first, 0)
            load(NWI[layer]).wait()
            r.NPRE[...] = dot(node, nw[0:D])
        with scope("f_halo_wait"):
            load(EWO[layer]).wait()
            load(NWO[layer]).wait()
            all_rows.wait()
        with scope("f_edges"):
            if layer == 0:
                load(12).wait()
                load(13).wait()
            gain = eg[layer : layer + 1, :]
            ps[HALO_AT : HALO_AT + HALO] = dot(r.HR[layer][...], w[D : 2 * D]).astype(BF)

            def edges(t, carry):
                at = tile_at(t, FORE)
                pre_act = r.PRE[at] + dot(r.SR[at, HALO_AT:], ps[HALO_AT:])
                hidden, slope = swish(pre_act)
                hidden = hidden.astype(BF)
                r.H[layer][at] = hidden
                r.DA[layer][at] = slope.astype(BF)
                normed, inv_std = norm(dot(hidden, wo[...]))
                r.INV[layer][at] = inv_std
                r.N[layer][at] = normed.astype(BF)
                if layer == 0:
                    r.EB1[at] = (r.el[at].astype(F32) + normed * gain).astype(BF)
                return carry

            lax.fori_loop(0, EDGES // FORE, edges, 0, unroll=FORE_UNROLL)
        with scope("f_node"):
            agg = (dot(r.SRT[RECV_AT:HALO_AT], r.N[layer][...]) * gain).astype(BF)
            r.AGG[layer][...] = agg
            pre_act = r.NPRE[...] + dot(agg, nw[D:])
            hidden, slope = swish(pre_act)
            hidden = hidden.astype(BF)
            r.NH[layer][...] = hidden
            r.NDA[layer][...] = slope
            normed, inv_std = norm(dot(hidden, nwo[...]))
            r.NN[layer][...] = normed
            r.NINV[layer][...] = inv_std
            update = normed * ng[layer : layer + 1, :]
            if layer == 0:
                state = r.nl[...].astype(F32) + update
                r.V1[...] = state
                r.VB1[...] = state.astype(BF)
            else:
                r.OUT[0:NODES] = r.V1[...] + update

    def norm_back(grad, normed, inv_std):
        return inv_std * (
            grad
            - jnp.mean(grad, axis=-1, keepdims=True)
            - normed * jnp.mean(grad * normed, axis=-1, keepdims=True)
        )

    def fold_rows(a):
        return jnp.sum(a.reshape(a.shape[0] // 8, 8, a.shape[1]), axis=0)

    def backward_nodes(layer):
        nw = r.nwi.at[layer]
        node = vb(layer)[...]
        with scope("b_node"):
            grad = r.GV[...]
            normed = r.NN[layer][...]
            gain_sum = jnp.sum(grad * normed, axis=0, keepdims=True)
            gz = norm_back(grad * ng[layer : layer + 1, :], normed, r.NINV[layer][...]).astype(BF)
            ga = (dot_tb(gz, r.nwo[layer]) * r.NDA[layer][...]).astype(BF)
            grad_agg = dot_tb(ga, nw[D:]).astype(BF)
            r.GACC[...] = jnp.zeros((8, D), F32)

        def weights():
            with scope("b_dwn"):
                r.WN[0:D] = dot_ta(node, ga)
                r.WN[D:] = dot_ta(r.AGG[layer][...], ga)
                r.WNO[...] = dot_ta(r.NH[layer][...], gz)
                r.GV[...] = r.GV[...] + dot_tb(ga, nw[0:D])

        return grad_agg, gain_sum, weights

    def backward_edges(layer, grad_agg):
        wo = r.ewo.at[layer]
        gain = eg[layer : layer + 1, :]

        def edges(t, carry):
            at = tile_at(t, BACK)
            gm = dot(r.SR[at, RECV_AT:HALO_AT], grad_agg)
            if layer == 0:
                gm = gm + r.PRE[at]
            en = r.N[layer][at].astype(F32)
            r.GACC[...] += fold_rows(gm * en)
            ez = norm_back(gm * gain, en, r.INV[layer][at]).astype(BF)
            r.GZ[at] = ez
            ea = (dot_tb(ez, wo[...]) * r.DA[layer][at].astype(F32)).astype(BF)
            r.GA[at] = ea
            return carry

        with scope("b_edges"):
            lax.fori_loop(0, EDGES // BACK, edges, 0, unroll=BACK_UNROLL)

    def return_halo(layer):
        with scope("b_gsr"):
            sums = dot(r.SRT[...], r.GA[...])
            r.GSR[...] = sums[0:HALO_AT]
            r.BS[layer][...] = sums[HALO_AT : HALO_AT + HALO].astype(BF)
            copies, all_rows = halo_copies(layer, 1)
            for copy in copies:
                copy.start()
        return all_rows

    def edge_weights(layer):
        node = vb(layer)[...]
        with scope("b_dwe"):
            r.WE[0:D] = dot_ta(eb(layer)[...], r.GA[...])
            r.WEO[...] = dot_ta(r.H[layer][...], r.GZ[...])
            to_sender = r.GSR[0:NODES].astype(BF)
            to_receiver = r.GSR[RECV_AT:HALO_AT].astype(BF)
            r.WE[D : 2 * D] = dot_ta(node, to_sender) + dot_ta(r.HR[layer][...], r.BS[layer][...])
            r.WE[2 * D :] = dot_ta(node, to_receiver)
        return jnp.sum(r.GACC[...], axis=0, keepdims=True)

    def edge_inputs(layer):
        with scope("b_inputs"):
            to_receiver = r.GSR[RECV_AT:HALO_AT].astype(BF)
            r.GV[...] = r.GV[...] + dot_tb(to_receiver, r.ewi[layer, 2 * D :])
            if layer == 1:
                r.PRE[...] = dot_tb(r.GA[...], r.ewi[layer, 0:D])

    def take_halo(layer, copies):
        w = r.ewi.at[layer]
        with scope("b_halo_wait"):
            copies.wait()
        with scope("b_tail"):
            to_sender = (r.GSR[0:NODES] + dot(r.LT[...], r.BR[layer][...])).astype(BF)
            total = r.GV[...] + dot_tb(to_sender, w[D : 2 * D])
            r.GV[...] = total
        return total

    low = iota((8, D), 0) < 4

    def each_pair(make):
        def slab(zz, carry):
            for xx in range(4):
                for cc in range(2):
                    for yy in range(2):
                        make((zz, xx, cc), 2 * yy, (zz, (xx * 2 + cc) * 2 + yy))
            return carry

        lax.fori_loop(0, 4, slab, 0)

    def pair_rows(ref, k, start, size):
        zz, inner = k
        return ref[pl.ds(pl.multiple_of(zz * 16 * size, 8) + inner * size + start, 8), :]

    def edge_slots(k):
        e0, e1, e2 = (pair_rows(r.WE, k, 8 * i, 24) for i in range(3))
        out = pltpu.roll(pair_rows(r.WEO, k, 0, 8), 4, 0)
        return (e0, jnp.where(low, e1, out)), (e2, jnp.where(low, out, e1))

    def assemble_edges(layer, gain_sum):
        def pair(where, yy, k):
            for odd, (g0, g1) in enumerate(edge_slots(k)):
                at = where + (yy + odd,)
                if layer == 1:
                    both = jnp.concatenate([g0, g1], axis=0).astype(BF)
                    r.G[0, 0][at] = both[:, 0:384]
                    r.G[0, 2][at + (slice(0, 16),)] = both[:, 384:]
                else:
                    r.G[2, 0][at] = g0[:, 0:384].astype(BF)
                    r.G[2, 1][at] = g1[:, 0:384].astype(BF)
                    r.G[2, 2][at] = jnp.concatenate([g0[:, 384:], g1[:, 384:], gains], axis=0).astype(BF)

        if layer == 0:
            lanes = [gain_sum[:, 128 * i : 128 * (i + 1)] for i in range(4)]
            gains = jnp.zeros((8, 128), F32)
            for i in range(4):
                gains = jnp.where(iota((8, 128), 0) == i, lanes[i], gains)
        with scope("asm_edges"):
            each_pair(pair)

    def assemble_nodes(layer, *gain_sums):
        row = iota((8, D), 0) % 4
        gains = jnp.zeros((8, D), F32)
        for i, gain_sum in enumerate(gain_sums):
            gains = jnp.where(row == i, gain_sum, gains)
        def pair(where, yy, k):
            n0, n1 = (pair_rows(r.WN, k, 8 * i, 16) for i in range(2))
            last = pair_rows(r.WNO, k, 0, 8)
            slots = ((n0, jnp.where(low, last, gains)), (n1, jnp.where(low, gains, last)))
            for odd, (g2, g3) in enumerate(slots):
                at = where + (yy + odd,)
                if layer == 1:
                    both = jnp.concatenate([g2, g3], axis=0).astype(BF)
                    r.G[0, 1][at] = both[:, 0:384]
                    r.G[0, 2][at + (slice(16, 32),)] = both[:, 384:]
                else:
                    r.G[1, 0][at] = g2[:, 0:384].astype(BF)
                    r.G[1, 1][at] = g3[:, 0:384].astype(BF)
                    r.G[1, 2][at] = jnp.concatenate([g2[:, 384:], g3[:, 384:]], axis=0).astype(BF)

        with scope("asm_nodes"):
            each_pair(pair)

    def rs_copy(key, number, src, dst, device):
        return remote(src, dst, r.rs_send.at[key[0], key[1], number], r.rs_recv.at[key[0], key[1], number], device)

    def settle(key, number, ref):
        rs_copy(key, number, ref, ref, other_core).wait()

    def cores(key):
        return rs_copy(key, 0, r.G[key].at[:, :, 1 - core], r.RC[key], other_core)

    def axes(key):
        first, second, third = PART_ORDER[key[1]]
        return first, second, third, second - (1 if first < second else 0)

    def cut(key, first_at, half):
        first, second, _, _ = axes(key)
        index = [slice(None)] * 3
        index[first] = first_at
        index[second] = pl.ds(2 * half, 2)
        return tuple(index)

    def ring(key, slot):
        axis = axes(key)[0]
        me = place[axis]
        way, kind = slot // 3, slot % 3
        sign = 1 - 2 * way
        if kind == 0:
            src = r.RC[key].at[cut(key, wrap(me + 2, 4), 1 - way)]
        elif kind == 1:
            src = r.RC[key].at[cut(key, wrap(me + sign, 4), way)]
        else:
            src = r.CA[key].at[way]
        return rs_copy(key, 1 if kind == 0 else 2, src, r.RA[key].at[slot], peer(axis, sign))

    def second_copies(key):
        _, axis, _, at = axes(key)
        copies = []
        for step in (2, 1, 3):
            src = r.AB[key].at[(slice(None),) * at + (wrap(place[axis] + step, 4),)]
            copies.append(rs_copy(key, 3, src, r.RB[key].at[step - 1], peer(axis, step)))
        return copies

    def third_copies(key):
        axis = axes(key)[2]
        copies = []
        for step in (2, 1, 3):
            src = r.AD[key].at[wrap(place[axis] + step, 4)]
            copies.append(rs_copy(key, 4, src, r.RD[key].at[step - 1], peer(axis, step)))
        return copies

    def rs_cores(key):
        cores(key).start()

    def rs_ring(key):
        with scope("rs_ring"):
            cores(key).wait()
            mine, both = r.G[key], r.RC[key]

            def add(i, carry):
                both[i] = both[i] + mine[i, :, core]
                return carry

            lax.fori_loop(0, 4, add, 0)
            for slot in (0, 3, 1, 4):
                ring(key, slot).start()

    def rs_sums(key):
        with scope("rs_sums"):
            me = place[axes(key)[0]]
            got = r.RA[key]
            settle(key, 1, got.at[0:2])
            for way, sign in ((0, 1), (1, -1)):
                own = r.RC[key][cut(key, wrap(me + sign, 4), 1 - way)]
                r.CA[key][way] = own + got[3 * way]
                ring(key, 3 * way + 2).start()

    def rs_second(key):
        with scope("rs_second"):
            first, axis, _, at = axes(key)
            got = r.RA[key]
            settle(key, 2, got.at[0:4])
            for half in range(2):
                near, summed = (1, 5) if half == 0 else (4, 2)
                total = r.RC[key][cut(key, place[first], half)].astype(F32)
                total = total + got[near].astype(F32) + got[summed].astype(F32)
                index = (slice(None),) * at + (slice(2 * half, 2 * half + 2),)
                r.AB[key][index] = total.astype(BF)
            for copy in second_copies(key):
                copy.start()

    def rs_third(key):
        with scope("rs_third"):
            _, axis, _, at = axes(key)
            settle(key, 3, r.RB[key])
            total = r.AB[key][(slice(None),) * at + (place[axis],)].astype(F32)
            for i in range(3):
                total = total + r.RB[key][i].astype(F32)
            r.AD[key][...] = total.astype(BF)
            for copy in third_copies(key):
                copy.start()

    def rs_finish(key):
        with scope("rs_finish"):
            settle(key, 4, r.RD[key])
            total = r.AD[key][place[axes(key)[2]]].astype(F32)
            for i in range(3):
                total = total + r.RD[key][i].astype(F32)
            stream, part = key
            start = SUMS_AT + (0, 32, 48)[stream]
            rows = 16 if stream == 0 else 8
            if part < 2:
                r.OUT[start + rows * part : start + rows * part + rows, 0:384] = total
            else:
                r.OUT[start : start + 2 * rows, 384:] = total[0 : 2 * rows]
            if key == (2, 2):
                r.OUT[SUMS_AT + 64 :, 0:128] = total[16:24]

    def store(number):
        rows = pl.ds((0, NODES, SUMS_AT)[number], (NODES, NODES, 72)[number])
        return pltpu.make_async_copy(r.OUT.at[rows], out.at[rows], r.store.at[number])

    def each(call, stream, *parts):
        for part in parts or range(3):
            call((stream, part))

    forward(0)
    forward(1)
    store(0).start()
    load(COT).wait()
    r.GV[...] = r.cot[...].astype(F32)

    grad_agg, node_gain, node_weights = backward_nodes(1)
    backward_edges(1, grad_agg)
    copies = return_halo(1)
    edge_gain = edge_weights(1)
    assemble_edges(1, None)
    each(rs_cores, 0, 0)
    node_weights()
    assemble_nodes(1, edge_gain, node_gain)
    each(rs_cores, 0, 1, 2)
    edge_inputs(1)
    take_halo(1, copies)

    grad_agg, node_gain, node_weights = backward_nodes(0)
    each(rs_ring, 0, 0)
    node_weights()
    assemble_nodes(0, node_gain)
    each(rs_cores, 1)
    each(rs_ring, 0, 1, 2)
    backward_edges(0, grad_agg)
    copies = return_halo(0)
    each(rs_ring, 1)
    edge_gain = edge_weights(0)
    assemble_edges(0, edge_gain)
    each(rs_cores, 2)
    each(rs_sums, 0)
    edge_inputs(0)
    each(rs_ring, 2)
    each(rs_sums, 1)
    each(rs_second, 0)
    each(rs_sums, 2)
    each(rs_second, 1)
    r.OUT[NODES : 2 * NODES] = take_halo(0, copies)
    store(1).start()
    each(rs_third, 0)
    each(rs_second, 2)
    each(rs_third, 1)
    each(rs_third, 2)
    for stream in range(3):
        each(rs_finish, stream)
    with scope("z_store"):
        store(2).start()
        for number in range(3):
            store(number).wait()


def finish_kernel(sums, o_node, o_grad, o_ei, o_eo, o_ni, o_no, o_eg, o_ng):
    y = lax.axis_index(AXES[1])
    column = (lax.axis_index(AXES[0]) * SAMPLES + y) * 4
    is_even = lax.rem(y, 2) == 0
    o_node[...] = sums[0:NODES]
    o_grad[...] = sums[NODES : 2 * NODES]

    def edge_rows(layer, g0, g1):
        even = jnp.concatenate([g0, g1[0:4]], axis=0)
        odd = jnp.concatenate([g1[4:8], g0], axis=0)
        o_ei[:, layer] = jnp.where(is_even, even, odd)
        o_eo[layer] = jnp.where(is_even, g1[4:8], g1[0:4])

    def node_rows(layer, total):
        o_ni[layer] = total[0:8]
        last = total[8:16]
        o_no[layer] = jnp.where(is_even, last[0:4], last[4:8])
        return jnp.where(is_even, last[4:8], last[0:4])

    def four(row):
        lane = iota((1, D), 1)
        at = iota((1, 4), 1)
        picked = jnp.zeros((1, 4), F32)
        for i in range(4):
            value = jnp.sum(jnp.where(lane == column + i, row, 0.0), axis=1, keepdims=True)
            picked = jnp.where(at == i, value, picked)
        return picked

    def rows(start, size):
        return sums[SUMS_AT + start : SUMS_AT + start + size]

    edge_rows(1, rows(0, 8), rows(8, 8))
    edge_rows(0, rows(48, 8), rows(56, 8))
    gains = node_rows(1, rows(16, 16))
    o_eg[1:2] = four(gains[0:1])
    o_ng[1:2] = four(gains[1:2])
    o_ng[0:1] = four(node_rows(0, rows(32, 16))[0:1])
    last = rows(64, 8)
    o_eg[0:1] = four(jnp.concatenate([last[i : i + 1, 0:128] for i in range(4)], axis=1))


def body(*args):
    (node_latent, edge_latent, node_cotangent, ewi, ewo, nwi, nwo, *gains, edge_slot, edge_receiver, send_list, edge_count) = args
    vmem = pl.BlockSpec(memory_space=pltpu.VMEM)
    far = pl.BlockSpec(memory_space=pl.ANY)
    results = pl.pallas_call(
        kernel,
        out_shape=jax.ShapeDtypeStruct((SUMS_AT + 72, D), F32),
        in_specs=[far] * 13,
        out_specs=far,
        scratch_shapes=flat_scratch()[0],
        compiler_params=pltpu.CompilerParams(
            collective_id=0, has_side_effects=True, vmem_limit_bytes=VMEM_LIMIT
        ),
        cost_estimate=pl.CostEstimate(flops=10**10, bytes_accessed=10**7, transcendentals=10**6),
    )(
        node_latent[0],
        edge_latent[0],
        ewi,
        ewo,
        nwi,
        nwo,
        node_cotangent[0],
        edge_count,
        *gains,
        edge_slot.reshape(8, 128),
        edge_receiver.reshape(8, 128),
        send_list,
    )
    outs = (
        (NODES, D),
        (NODES, D),
        (12, 2, D),
        (2, 4, D),
        (2, 8, D),
        (2, 4, D),
        (2, 4),
        (2, 4),
    )
    results = pl.pallas_call(
        finish_kernel,
        out_shape=tuple(jax.ShapeDtypeStruct(shape, F32) for shape in outs),
        in_specs=[vmem],
        out_specs=tuple([vmem] * 8),
        compiler_params=pltpu.CompilerParams(vmem_limit_bytes=VMEM_LIMIT),
    )(results)
    return (results[0][None], results[1][None], jnp.transpose(results[2], (1, 0, 2))) + tuple(results[3:])


def solution(mesh):
    nodes = P(AXES[1], AXES[0], None)
    graph = P(AXES[0])
    in_specs = (nodes, nodes, nodes) + (P(),) * 6 + (graph, graph, P(AXES[0], None), graph)
    rows = P(None, AXES, None)
    out_specs = (nodes, nodes) + (rows,) * 4 + (P(None, AXES),) * 2
    return jax.shard_map(body, mesh=mesh, in_specs=in_specs, out_specs=out_specs, check_vma=False)
```

```python
import types

import jax
import jax.numpy as jnp
from jax import lax
from jax.experimental import pallas as pl
from jax.experimental.pallas import tpu as pltpu
from jax.sharding import PartitionSpec as P

HOPS = 2
EPSILON = 1e-05
BF = jnp.bfloat16
F32 = jnp.float32
D = 512
NODES = 128
EDGES = 1024
PEER = 32
GROUP = 32
SAMPLES = 4
VMEM_LIMIT = 62 * 1024 * 1024
OFFSETS = tuple(o for o in range(-HOPS, HOPS + 1) if o != 0) + (GROUP // 2,)
HALO = len(OFFSETS) * PEER
RECV_AT = NODES
HALO_AT = 2 * NODES
SUMS_AT = 2 * NODES
FIRST, FORE, BACK = 1024, 1024, 1024
FORE_UNROLL, BACK_UNROLL = 1, 1
MESH = pl.DeviceIdType.MESH
STREAM_TILES = (
    ((16, 384), (16, 384), (32, 128)),
    ((8, 384), (8, 384), (16, 128)),
    ((8, 384), (8, 384), (24, 128)),
)
PART_ORDER = ((1, 2, 0), (2, 0, 1), (0, 1, 2))
AXES = ("graph", "batch")
scope = jax.named_scope


def dot(a, b):
    return jnp.dot(a, b, preferred_element_type=F32)


def dot_tb(a, b):
    return lax.dot_general(a, b, (((1,), (1,)), ((), ())), preferred_element_type=F32)


def dot_ta(a, b):
    return lax.dot_general(a, b, (((0,), (0,)), ((), ())), preferred_element_type=F32)


def place_id(graph, batch):
    return dict(zip(AXES, (graph, batch)))


def wrap(value, size):
    return lax.rem(value + 2 * size, size)


def iota(shape, dim):
    return lax.broadcasted_iota(jnp.int32, shape, dim)


def half_shape(part):
    first, second, _ = PART_ORDER[part]
    shape = [4, 4, 4]
    shape[second] = 2
    del shape[first]
    return tuple(shape)


NL, EWI, EL, EWO, NWI, NWO, COT = 0, (1, 6), 2, (3, 7), (4, 8), (5, 9), 10


def scratch_spec():
    vm = pltpu.VMEM

    def two(shape, dtype):
        return [vm(shape, dtype), vm(shape, dtype)]

    def parts(shape):
        keys = [(stream, part) for stream in range(3) for part in range(3)]
        return {key: vm(shape(key[1]) + STREAM_TILES[key[0]][key[1]], BF) for key in keys}

    return dict(
        nl=vm((NODES, D), BF),
        el=vm((EDGES, D), BF),
        ewi=vm((2, 3 * D, D), BF),
        ewo=vm((2, D, D), BF),
        nwi=vm((2, 2 * D, D), BF),
        nwo=vm((2, D, D), BF),
        cot=vm((NODES, D), BF),
        cnt=pltpu.SMEM((1,), jnp.int32),
        small=[
            vm((2, D), F32),
            vm((2, D), F32),
            vm((8, 128), jnp.int32),
            vm((8, 128), jnp.int32),
            vm((GROUP, PEER), jnp.int32),
        ],
        SR=vm((EDGES, 512), BF),
        SRT=vm((512, EDGES), BF),
        LT=vm((NODES, HALO), BF),
        PS=vm((512, D), BF),
        PRE=vm((EDGES, D), F32),
        EB1=vm((EDGES, D), BF),
        VB1=vm((NODES, D), BF),
        V1=vm((NODES, D), F32),
        NPRE=vm((NODES, D), F32),
        N=two((EDGES, D), BF),
        DA=two((EDGES, D), BF),
        H=two((EDGES, D), BF),
        INV=two((EDGES, 1), F32),
        NN=two((NODES, D), F32),
        NDA=two((NODES, D), F32),
        NH=two((NODES, D), BF),
        NINV=two((NODES, 1), F32),
        AGG=two((NODES, D), BF),
        HS=two((HALO, D), BF),
        HR=two((HALO, D), BF),
        BS=two((HALO, D), BF),
        BR=two((HALO, D), BF),
        G=parts(lambda part: (4, 4, 2, 4)),
        RC=parts(lambda part: (4, 4, 4)),
        RA=parts(lambda part: (6,) + half_shape(part)),
        CA=parts(lambda part: (2,) + half_shape(part)),
        AB=parts(lambda part: (4, 4)),
        RB=parts(lambda part: (3, 4)),
        AD=parts(lambda part: (4,)),
        RD=parts(lambda part: (3,)),
        GZ=vm((EDGES, D), BF),
        GA=vm((EDGES, D), BF),
        GSR=vm((HALO_AT, D), F32),
        GV=vm((NODES, D), F32),
        GACC=vm((8, D), F32),
        WE=vm((3 * D, D), F32),
        WEO=vm((D, D), F32),
        WN=vm((2 * D, D), F32),
        WNO=vm((D, D), F32),
        OUT=vm((SUMS_AT + 72, D), F32),
        store=pltpu.SemaphoreType.DMA((3,)),
        load=pltpu.SemaphoreType.DMA((17,)),
        halo_send=pltpu.SemaphoreType.DMA((2, 2)),
        halo_recv=pltpu.SemaphoreType.DMA((2, 2)),
        rs_send=pltpu.SemaphoreType.DMA((3, 3, 4)),
        rs_recv=pltpu.SemaphoreType.DMA((3, 3, 5)),
    )


def flat_scratch():
    return jax.tree.flatten(scratch_spec())


def kernel(*refs):
    far, out = refs[:13], refs[13]
    r = types.SimpleNamespace(**jax.tree.unflatten(flat_scratch()[1], refs[14:]))
    g = lax.axis_index(AXES[0])
    y = lax.axis_index(AXES[1])
    core = lax.rem(g, 2)
    x = lax.rem(g // 2, 4)
    z = g // 8
    place = (z, x, y)

    def peer(axis, step):
        zz = wrap(z + step, 4) if axis == 0 else z
        xx = wrap(x + step, 4) if axis == 1 else x
        yy = wrap(y + step, 4) if axis == 2 else y
        return place_id((zz * 4 + xx) * 2 + core, yy)

    def graph_peer(offset):
        return place_id(wrap(g + offset, GROUP), y)

    other_core = place_id(g + 1 - 2 * core, y)

    nl, el, ewi, ewo, nwi, nwo, cot, cnt, *small = far
    pairs = [(nl, r.nl), (ewi, r.ewi, 0), (el, r.el), (ewo, r.ewo, 0), (nwi, r.nwi, 0), (nwo, r.nwo, 0)]
    pairs += [(ewi, r.ewi, 1), (ewo, r.ewo, 1), (nwi, r.nwi, 1), (nwo, r.nwo, 1), (cot, r.cot), (cnt, r.cnt)]
    eg, ng, slot, rcv, slist = r.small
    pairs += list(zip(small, r.small))

    def load(number):
        src, dst, *layer = pairs[number]
        if layer:
            src, dst = src.at[layer[0]], dst.at[layer[0]]
        return pltpu.make_async_copy(src, dst, r.load.at[number])

    for number in (16, 0):
        load(number).start()

    barrier = pltpu.get_barrier_semaphore()
    greeted = 0
    for offset in OFFSETS:
        pl.semaphore_signal(barrier, inc=1, device_id=graph_peer(offset), device_id_type=MESH)
        pl.semaphore_signal(barrier, inc=1, device_id=graph_peer(-offset), device_id_type=MESH)
        greeted += 2
    for axis in range(3):
        for step in (1, 2, 3):
            pl.semaphore_signal(barrier, inc=1, device_id=peer(axis, step), device_id_type=MESH)
            greeted += 1
    pl.semaphore_signal(barrier, inc=1, device_id=other_core, device_id_type=MESH)
    greeted += 1

    for number in (14, 15, 11) + tuple(range(1, 11)) + (12, 13):
        load(number).start()

    load(16).wait()
    listed = jnp.concatenate(
        [slist[pl.ds(wrap(g - offset, GROUP), 1), :] for offset in OFFSETS], axis=1
    ).astype(F32)
    node_ids = iota((NODES, HALO), 0).astype(F32)
    r.LT[...] = jnp.where(node_ids == listed, 1.0, 0.0).astype(BF)

    def remote(src, dst, send_sem, recv_sem, device):
        return pltpu.make_async_remote_copy(
            src_ref=src,
            dst_ref=dst,
            send_sem=send_sem,
            recv_sem=recv_sem,
            device_id=device,
            device_id_type=MESH,
        )

    def halo_copies(layer, way):
        src, dst = ((r.HS, r.HR), (r.BS, r.BR))[way]
        src, dst = src[layer], dst[layer]
        copies = []
        for b in reversed(range(len(OFFSETS))):
            offset = OFFSETS[b]
            rows = pl.ds(b * PEER, PEER)
            copies.append(
                remote(
                    src.at[rows],
                    dst.at[rows],
                    r.halo_send.at[layer, way],
                    r.halo_recv.at[layer, way],
                    graph_peer(-offset if way == 0 else offset),
                )
            )
        return copies, remote(src, dst, r.halo_send.at[layer, way], r.halo_recv.at[layer, way], other_core)

    def vb(layer):
        return r.nl if layer == 0 else r.VB1

    def eb(layer):
        return r.el if layer == 0 else r.EB1

    def one_hots():
        for number in (11, 14, 15):
            load(number).wait()
        s = slot[...]
        within = s - NODES
        source = within // PEER
        distance = wrap(source - g, GROUP)
        block = jnp.zeros_like(s)
        for b, offset in enumerate(OFFSETS):
            block = jnp.where(distance == offset % GROUP, b, block)
        position = jnp.where(s < NODES, s, HALO_AT + block * PEER + (within - source * PEER))
        edge = iota((8, 128), 0) * 128 + iota((8, 128), 1)
        receiver = jnp.where(edge < r.cnt[0], rcv[...] + RECV_AT, -1)
        position = position.astype(F32)
        receiver = receiver.astype(F32)
        row_ids = iota((512, 128), 0).astype(F32)
        lane_ids = iota((128, 512), 1).astype(F32)
        for i in range(8):
            prow = position[i : i + 1, :]
            rrow = receiver[i : i + 1, :]
            at = slice(i * 128, (i + 1) * 128)
            for j in range(4):
                rows = slice(j * 128, (j + 1) * 128)
                row = rrow if j == 1 else prow
                r.SRT[rows, at] = jnp.where(row_ids[rows] == row, 1.0, 0.0).astype(BF)
            pcol = jnp.broadcast_to(prow, (128, 128)).T
            rcol = jnp.broadcast_to(rrow, (128, 128)).T
            for j in range(4):
                col = rcol if j == 1 else pcol
                lanes = slice(j * 128, (j + 1) * 128)
                r.SR[at, lanes] = jnp.where(lane_ids[:, lanes] == col, 1.0, 0.0).astype(BF)

    def norm(projected):
        centre = projected - jnp.mean(projected, axis=-1, keepdims=True)
        inv_std = lax.rsqrt(jnp.mean(centre * centre, axis=-1, keepdims=True) + EPSILON)
        return centre * inv_std, inv_std

    def swish(pre_act):
        sigma = 0.5 * jnp.tanh(0.5 * pre_act) + 0.5
        hidden = pre_act * sigma
        return hidden, sigma + hidden * (1.0 - sigma)

    def tile_at(t, rows):
        return pl.ds(pl.multiple_of(t * rows, rows), rows)

    def forward(layer):
        w = r.ewi.at[layer]
        wo = r.ewo.at[layer]
        nw = r.nwi.at[layer]
        nwo = r.nwo.at[layer]
        ps = r.PS
        with scope("f_send"):
            if layer == 0:
                load(NL).wait()
            r.HS[layer][...] = dot_ta(r.LT[...], vb(layer)[...]).astype(BF)
            copies, all_rows = halo_copies(layer, 0)
            if layer == 0:
                pl.semaphore_wait(barrier, greeted)
            for copy in copies:
                copy.start()
        with scope("f_first"):
            if layer == 0:
                one_hots()
            node = vb(layer)[...]
            load(EWI[layer]).wait()
            ps[0:NODES] = dot(node, w[D : 2 * D]).astype(BF)
            ps[RECV_AT:HALO_AT] = dot(node, w[2 * D :]).astype(BF)
            if layer == 0:
                ps[HALO_AT + HALO :] = jnp.zeros((512 - HALO_AT - HALO, D), BF)
                load(EL).wait()

            def first(t, carry):
                at = tile_at(t, FIRST)
                r.PRE[at] = dot(eb(layer)[at], w[0:D]) + dot(r.SR[at, 0:HALO_AT], ps[0:HALO_AT])
                return carry

            lax.fori_loop(0, EDGES // FIRST, first, 0)
            load(NWI[layer]).wait()
            r.NPRE[...] = dot(node, nw[0:D])
        with scope("f_halo_wait"):
            load(EWO[layer]).wait()
            load(NWO[layer]).wait()
            all_rows.wait()
        with scope("f_edges"):
            if layer == 0:
                load(12).wait()
                load(13).wait()
            gain = eg[layer : layer + 1, :]
            ps[HALO_AT : HALO_AT + HALO] = dot(r.HR[layer][...], w[D : 2 * D]).astype(BF)

            def edges(t, carry):
                at = tile_at(t, FORE)
                pre_act = r.PRE[at] + dot(r.SR[at, HALO_AT:], ps[HALO_AT:])
                hidden, slope = swish(pre_act)
                hidden = hidden.astype(BF)
                r.H[layer][at] = hidden
                r.DA[layer][at] = slope.astype(BF)
                normed, inv_std = norm(dot(hidden, wo[...]))
                r.INV[layer][at] = inv_std
                r.N[layer][at] = normed.astype(BF)
                if layer == 0:
                    r.EB1[at] = (r.el[at].astype(F32) + normed * gain).astype(BF)
                return carry

            lax.fori_loop(0, EDGES // FORE, edges, 0, unroll=FORE_UNROLL)
        with scope("f_node"):
            agg = (dot(r.SRT[RECV_AT:HALO_AT], r.N[layer][...]) * gain).astype(BF)
            r.AGG[layer][...] = agg
            pre_act = r.NPRE[...] + dot(agg, nw[D:])
            hidden, slope = swish(pre_act)
            hidden = hidden.astype(BF)
            r.NH[layer][...] = hidden
            r.NDA[layer][...] = slope
            normed, inv_std = norm(dot(hidden, nwo[...]))
            r.NN[layer][...] = normed
            r.NINV[layer][...] = inv_std
            update = normed * ng[layer : layer + 1, :]
            if layer == 0:
                state = r.nl[...].astype(F32) + update
                r.V1[...] = state
                r.VB1[...] = state.astype(BF)
            else:
                r.OUT[0:NODES] = r.V1[...] + update

    def norm_back(grad, normed, inv_std):
        return inv_std * (
            grad
            - jnp.mean(grad, axis=-1, keepdims=True)
            - normed * jnp.mean(grad * normed, axis=-1, keepdims=True)
        )

    def fold_rows(a):
        return jnp.sum(a.reshape(a.shape[0] // 8, 8, a.shape[1]), axis=0)

    def backward_nodes(layer):
        nw = r.nwi.at[layer]
        node = vb(layer)[...]
        with scope("b_node"):
            grad = r.GV[...]
            normed = r.NN[layer][...]
            gain_sum = jnp.sum(grad * normed, axis=0, keepdims=True)
            gz = norm_back(grad * ng[layer : layer + 1, :], normed, r.NINV[layer][...]).astype(BF)
            ga = (dot_tb(gz, r.nwo[layer]) * r.NDA[layer][...]).astype(BF)
            grad_agg = dot_tb(ga, nw[D:]).astype(BF)
            r.GACC[...] = jnp.zeros((8, D), F32)

        def weights():
            with scope("b_dwn"):
                r.WN[0:D] = dot_ta(node, ga)
                r.WN[D:] = dot_ta(r.AGG[layer][...], ga)
                r.WNO[...] = dot_ta(r.NH[layer][...], gz)
                r.GV[...] = r.GV[...] + dot_tb(ga, nw[0:D])

        return grad_agg, gain_sum, weights

    def backward_edges(layer, grad_agg):
        wo = r.ewo.at[layer]
        gain = eg[layer : layer + 1, :]

        def edges(t, carry):
            at = tile_at(t, BACK)
            gm = dot(r.SR[at, RECV_AT:HALO_AT], grad_agg)
            if layer == 0:
                gm = gm + r.PRE[at]
            en = r.N[layer][at].astype(F32)
            r.GACC[...] += fold_rows(gm * en)
            ez = norm_back(gm * gain, en, r.INV[layer][at]).astype(BF)
            r.GZ[at] = ez
            ea = (dot_tb(ez, wo[...]) * r.DA[layer][at].astype(F32)).astype(BF)
            r.GA[at] = ea
            return carry

        with scope("b_edges"):
            lax.fori_loop(0, EDGES // BACK, edges, 0, unroll=BACK_UNROLL)

    def return_halo(layer):
        with scope("b_gsr"):
            sums = dot(r.SRT[...], r.GA[...])
            r.GSR[...] = sums[0:HALO_AT]
            r.BS[layer][...] = sums[HALO_AT : HALO_AT + HALO].astype(BF)
            copies, all_rows = halo_copies(layer, 1)
            for copy in copies:
                copy.start()
        return all_rows

    def edge_weights(layer):
        node = vb(layer)[...]
        with scope("b_dwe"):
            r.WE[0:D] = dot_ta(eb(layer)[...], r.GA[...])
            r.WEO[...] = dot_ta(r.H[layer][...], r.GZ[...])
            to_sender = r.GSR[0:NODES].astype(BF)
            to_receiver = r.GSR[RECV_AT:HALO_AT].astype(BF)
            r.WE[D : 2 * D] = dot_ta(node, to_sender) + dot_ta(r.HR[layer][...], r.BS[layer][...])
            r.WE[2 * D :] = dot_ta(node, to_receiver)
        return jnp.sum(r.GACC[...], axis=0, keepdims=True)

    def edge_inputs(layer):
        with scope("b_inputs"):
            to_receiver = r.GSR[RECV_AT:HALO_AT].astype(BF)
            r.GV[...] = r.GV[...] + dot_tb(to_receiver, r.ewi[layer, 2 * D :])
            if layer == 1:
                r.PRE[...] = dot_tb(r.GA[...], r.ewi[layer, 0:D])

    def take_halo(layer, copies):
        w = r.ewi.at[layer]
        with scope("b_halo_wait"):
            copies.wait()
        with scope("b_tail"):
            to_sender = (r.GSR[0:NODES] + dot(r.LT[...], r.BR[layer][...])).astype(BF)
            total = r.GV[...] + dot_tb(to_sender, w[D : 2 * D])
            r.GV[...] = total
        return total

    low = iota((8, D), 0) < 4

    def each_pair(make):
        def slab(zz, carry):
            for xx in range(4):
                for cc in range(2):
                    for yy in range(2):
                        make((zz, xx, cc), 2 * yy, (zz, (xx * 2 + cc) * 2 + yy))
            return carry

        lax.fori_loop(0, 4, slab, 0)

    def pair_rows(ref, k, start, size):
        zz, inner = k
        return ref[pl.ds(pl.multiple_of(zz * 16 * size, 8) + inner * size + start, 8), :]

    def edge_slots(k):
        e0, e1, e2 = (pair_rows(r.WE, k, 8 * i, 24) for i in range(3))
        out = pltpu.roll(pair_rows(r.WEO, k, 0, 8), 4, 0)
        return (e0, jnp.where(low, e1, out)), (e2, jnp.where(low, out, e1))

    def assemble_edges(layer, gain_sum):
        def pair(where, yy, k):
            for odd, (g0, g1) in enumerate(edge_slots(k)):
                at = where + (yy + odd,)
                if layer == 1:
                    both = jnp.concatenate([g0, g1], axis=0).astype(BF)
                    r.G[0, 0][at] = both[:, 0:384]
                    r.G[0, 2][at + (slice(0, 16),)] = both[:, 384:]
                else:
                    r.G[2, 0][at] = g0[:, 0:384].astype(BF)
                    r.G[2, 1][at] = g1[:, 0:384].astype(BF)
                    r.G[2, 2][at] = jnp.concatenate([g0[:, 384:], g1[:, 384:], gains], axis=0).astype(BF)

        if layer == 0:
            lanes = [gain_sum[:, 128 * i : 128 * (i + 1)] for i in range(4)]
            gains = jnp.zeros((8, 128), F32)
            for i in range(4):
                gains = jnp.where(iota((8, 128), 0) == i, lanes[i], gains)
        with scope("asm_edges"):
            each_pair(pair)

    def assemble_nodes(layer, *gain_sums):
        row = iota((8, D), 0) % 4
        gains = jnp.zeros((8, D), F32)
        for i, gain_sum in enumerate(gain_sums):
            gains = jnp.where(row == i, gain_sum, gains)
        def pair(where, yy, k):
            n0, n1 = (pair_rows(r.WN, k, 8 * i, 16) for i in range(2))
            last = pair_rows(r.WNO, k, 0, 8)
            slots = ((n0, jnp.where(low, last, gains)), (n1, jnp.where(low, gains, last)))
            for odd, (g2, g3) in enumerate(slots):
                at = where + (yy + odd,)
                if layer == 1:
                    both = jnp.concatenate([g2, g3], axis=0).astype(BF)
                    r.G[0, 1][at] = both[:, 0:384]
                    r.G[0, 2][at + (slice(16, 32),)] = both[:, 384:]
                else:
                    r.G[1, 0][at] = g2[:, 0:384].astype(BF)
                    r.G[1, 1][at] = g3[:, 0:384].astype(BF)
                    r.G[1, 2][at] = jnp.concatenate([g2[:, 384:], g3[:, 384:]], axis=0).astype(BF)

        with scope("asm_nodes"):
            each_pair(pair)

    def rs_copy(key, number, src, dst, device):
        sent = (0, 1, 1, 2, 3)[number]
        return remote(src, dst, r.rs_send.at[key[0], key[1], sent], r.rs_recv.at[key[0], key[1], number], device)

    def settle(key, number, ref):
        rs_copy(key, number, ref, ref, other_core).wait()

    def cores(key):
        return rs_copy(key, 0, r.G[key].at[:, :, 1 - core], r.RC[key], other_core)

    def axes(key):
        first, second, third = PART_ORDER[key[1]]
        return first, second, third, second - (1 if first < second else 0)

    def cut(key, first_at, half):
        first, second, _, _ = axes(key)
        index = [slice(None)] * 3
        index[first] = first_at
        index[second] = pl.ds(2 * half, 2)
        return tuple(index)

    def ring(key, slot):
        axis = axes(key)[0]
        me = place[axis]
        way, kind = slot // 3, slot % 3
        sign = 1 - 2 * way
        if kind == 0:
            src = r.RC[key].at[cut(key, wrap(me + 2, 4), 1 - way)]
        elif kind == 1:
            src = r.RC[key].at[cut(key, wrap(me + sign, 4), way)]
        else:
            src = r.CA[key].at[way]
        return rs_copy(key, 1 if kind == 0 else 2, src, r.RA[key].at[slot], peer(axis, sign))

    def second_copies(key):
        _, axis, _, at = axes(key)
        copies = []
        for step in (2, 1, 3):
            src = r.AB[key].at[(slice(None),) * at + (wrap(place[axis] + step, 4),)]
            copies.append(rs_copy(key, 3, src, r.RB[key].at[step - 1], peer(axis, step)))
        return copies

    def third_copies(key):
        axis = axes(key)[2]
        copies = []
        for step in (2, 1, 3):
            src = r.AD[key].at[wrap(place[axis] + step, 4)]
            copies.append(rs_copy(key, 4, src, r.RD[key].at[step - 1], peer(axis, step)))
        return copies

    def rs_cores(key):
        cores(key).start()

    def rs_ring(key):
        with scope("rs_ring"):
            cores(key).wait()
            mine, both = r.G[key], r.RC[key]

            def add(i, carry):
                both[i] = both[i] + mine[i, :, core]
                return carry

            lax.fori_loop(0, 4, add, 0)
            for slot in (0, 3, 1, 4):
                ring(key, slot).start()

    def rs_sums(key):
        with scope("rs_sums"):
            me = place[axes(key)[0]]
            got = r.RA[key]
            rs_copy(key, 1, got.at[0:2], got.at[0:2], other_core).wait_recv()
            for way, sign in ((0, 1), (1, -1)):
                own = r.RC[key][cut(key, wrap(me + sign, 4), 1 - way)]
                r.CA[key][way] = own + got[3 * way]
                ring(key, 3 * way + 2).start()

    def rs_second(key):
        with scope("rs_second"):
            first, axis, _, at = axes(key)
            got = r.RA[key]
            rs_copy(key, 2, got.at[0:4], got.at[0:4], other_core).wait_recv()
            rs_copy(key, 2, got, got, other_core).wait_send()
            for half in range(2):
                near, summed = (1, 5) if half == 0 else (4, 2)
                total = r.RC[key][cut(key, place[first], half)].astype(F32)
                total = total + got[near].astype(F32) + got[summed].astype(F32)
                index = (slice(None),) * at + (slice(2 * half, 2 * half + 2),)
                r.AB[key][index] = total.astype(BF)
            for copy in second_copies(key):
                copy.start()

    def rs_third(key):
        with scope("rs_third"):
            _, axis, _, at = axes(key)
            settle(key, 3, r.RB[key])
            total = r.AB[key][(slice(None),) * at + (place[axis],)].astype(F32)
            for i in range(3):
                total = total + r.RB[key][i].astype(F32)
            r.AD[key][...] = total.astype(BF)
            for copy in third_copies(key):
                copy.start()

    def rs_finish(key):
        with scope("rs_finish"):
            settle(key, 4, r.RD[key])
            total = r.AD[key][place[axes(key)[2]]].astype(F32)
            for i in range(3):
                total = total + r.RD[key][i].astype(F32)
            stream, part = key
            start = SUMS_AT + (0, 32, 48)[stream]
            rows = 16 if stream == 0 else 8
            if part < 2:
                r.OUT[start + rows * part : start + rows * part + rows, 0:384] = total
            else:
                r.OUT[start : start + 2 * rows, 384:] = total[0 : 2 * rows]
            if key == (2, 2):
                r.OUT[SUMS_AT + 64 :, 0:128] = total[16:24]

    def store(number):
        rows = pl.ds((0, NODES, SUMS_AT)[number], (NODES, NODES, 72)[number])
        return pltpu.make_async_copy(r.OUT.at[rows], out.at[rows], r.store.at[number])

    def each(call, stream, *parts):
        for part in parts or range(3):
            call((stream, part))

    forward(0)
    forward(1)
    store(0).start()
    load(COT).wait()
    r.GV[...] = r.cot[...].astype(F32)

    grad_agg, node_gain, node_weights = backward_nodes(1)
    backward_edges(1, grad_agg)
    copies = return_halo(1)
    edge_gain = edge_weights(1)
    assemble_edges(1, None)
    each(rs_cores, 0, 0)
    node_weights()
    assemble_nodes(1, edge_gain, node_gain)
    each(rs_cores, 0, 1, 2)
    edge_inputs(1)
    take_halo(1, copies)

    grad_agg, node_gain, node_weights = backward_nodes(0)
    each(rs_ring, 0, 0)
    node_weights()
    assemble_nodes(0, node_gain)
    each(rs_cores, 1)
    each(rs_ring, 0, 1, 2)
    backward_edges(0, grad_agg)
    copies = return_halo(0)
    each(rs_ring, 1)
    edge_gain = edge_weights(0)
    assemble_edges(0, edge_gain)
    each(rs_cores, 2)
    each(rs_sums, 0)
    edge_inputs(0)
    each(rs_ring, 2)
    each(rs_sums, 1)
    each(rs_second, 0)
    each(rs_sums, 2)
    each(rs_second, 1)
    r.OUT[NODES : 2 * NODES] = take_halo(0, copies)
    store(1).start()
    each(rs_third, 0)
    each(rs_second, 2)
    each(rs_third, 1)
    each(rs_third, 2)
    for stream in range(3):
        each(rs_finish, stream)
    with scope("z_store"):
        store(2).start()
        for number in range(3):
            store(number).wait()


def finish_kernel(sums, o_node, o_grad, o_ei, o_eo, o_ni, o_no, o_eg, o_ng):
    y = lax.axis_index(AXES[1])
    column = (lax.axis_index(AXES[0]) * SAMPLES + y) * 4
    is_even = lax.rem(y, 2) == 0
    o_node[...] = sums[0:NODES]
    o_grad[...] = sums[NODES : 2 * NODES]

    def edge_rows(layer, g0, g1):
        even = jnp.concatenate([g0, g1[0:4]], axis=0)
        odd = jnp.concatenate([g1[4:8], g0], axis=0)
        o_ei[:, layer] = jnp.where(is_even, even, odd)
        o_eo[layer] = jnp.where(is_even, g1[4:8], g1[0:4])

    def node_rows(layer, total):
        o_ni[layer] = total[0:8]
        last = total[8:16]
        o_no[layer] = jnp.where(is_even, last[0:4], last[4:8])
        return jnp.where(is_even, last[4:8], last[0:4])

    def four(row):
        lane = iota((1, D), 1)
        at = iota((1, 4), 1)
        picked = jnp.zeros((1, 4), F32)
        for i in range(4):
            value = jnp.sum(jnp.where(lane == column + i, row, 0.0), axis=1, keepdims=True)
            picked = jnp.where(at == i, value, picked)
        return picked

    def rows(start, size):
        return sums[SUMS_AT + start : SUMS_AT + start + size]

    edge_rows(1, rows(0, 8), rows(8, 8))
    edge_rows(0, rows(48, 8), rows(56, 8))
    gains = node_rows(1, rows(16, 16))
    o_eg[1:2] = four(gains[0:1])
    o_ng[1:2] = four(gains[1:2])
    o_ng[0:1] = four(node_rows(0, rows(32, 16))[0:1])
    last = rows(64, 8)
    o_eg[0:1] = four(jnp.concatenate([last[i : i + 1, 0:128] for i in range(4)], axis=1))


def body(*args):
    (node_latent, edge_latent, node_cotangent, ewi, ewo, nwi, nwo, *gains, edge_slot, edge_receiver, send_list, edge_count) = args
    vmem = pl.BlockSpec(memory_space=pltpu.VMEM)
    far = pl.BlockSpec(memory_space=pl.ANY)
    results = pl.pallas_call(
        kernel,
        out_shape=jax.ShapeDtypeStruct((SUMS_AT + 72, D), F32),
        in_specs=[far] * 13,
        out_specs=far,
        scratch_shapes=flat_scratch()[0],
        compiler_params=pltpu.CompilerParams(
            collective_id=0, has_side_effects=True, vmem_limit_bytes=VMEM_LIMIT
        ),
        cost_estimate=pl.CostEstimate(flops=10**10, bytes_accessed=10**7, transcendentals=10**6),
    )(
        node_latent[0],
        edge_latent[0],
        ewi,
        ewo,
        nwi,
        nwo,
        node_cotangent[0],
        edge_count,
        *gains,
        edge_slot.reshape(8, 128),
        edge_receiver.reshape(8, 128),
        send_list,
    )
    outs = (
        (NODES, D),
        (NODES, D),
        (12, 2, D),
        (2, 4, D),
        (2, 8, D),
        (2, 4, D),
        (2, 4),
        (2, 4),
    )
    results = pl.pallas_call(
        finish_kernel,
        out_shape=tuple(jax.ShapeDtypeStruct(shape, F32) for shape in outs),
        in_specs=[vmem],
        out_specs=tuple([vmem] * 8),
        compiler_params=pltpu.CompilerParams(vmem_limit_bytes=VMEM_LIMIT),
    )(results)
    return (results[0][None], results[1][None], jnp.transpose(results[2], (1, 0, 2))) + tuple(results[3:])


def solution(mesh):
    nodes = P(AXES[1], AXES[0], None)
    graph = P(AXES[0])
    in_specs = (nodes, nodes, nodes) + (P(),) * 6 + (graph, graph, P(AXES[0], None), graph)
    rows = P(None, AXES, None)
    out_specs = (nodes, nodes) + (rows,) * 4 + (P(None, AXES),) * 2
    return jax.shard_map(body, mesh=mesh, in_specs=in_specs, out_specs=out_specs, check_vma=False)
```
